32 devices in a mesh: slab: 4 (over x, core), img: 8 (over z, y).
Axes of the slice: x: 2, y: 2, z: 4, core: 2. Of those that a mesh axis runs over, the one named last changes fastest.
Arguments:
- feats: bfloat16 [8, 32, 128, 512], P('img', 'slab'), may hold values from -6 to 6
- labels: int32 [8], P('img'), may hold values from 0 to 999
- conv_w: bfloat16 [9, 512, 4], replicated, may hold values from -0.09375 to 0.09375
- embed_w: bfloat16 [16, 1024], replicated, may hold values from -1.5 to 1.5
- mod_table: bfloat16 [1000, 2048], replicated, may hold values from -3 to 3
- qkv_w: bfloat16 [1024, 3072], replicated, may hold values from -0.1875 to 0.1875
- out_w: bfloat16 [1024, 1024], replicated, may hold values from -0.1875 to 0.1875
- proj_w: bfloat16 [1024, 768], replicated, may hold values from -0.1875 to 0.1875
- dino: bfloat16 [8, 1024, 768], P('img', 'slab'), may hold values from -6 to 6
Outputs:
- grad_feats: bfloat16 [8, 32, 128, 512], P('img', 'slab')
- grad_proj: float32 [1024, 768], replicated
- grad_conv: float32 [9, 512, 4], replicated
- loss: float32 [], replicated
The draws below stay inside these ranges and needn't reach their ends.
All inputs are finite; a program needn't handle non-finite values.
Results may differ from the reference program's by a relative error of at most 0.024.
Values may be sent and summed in bfloat16 or wider, within the bound.
A program may use at most 128 MiB of HBM per device.

```python
import jax
import jax.numpy as jnp
from jax import lax

C = 512
LAT = 4
D = 1024
HEAD_DIM = 64
DINO = 768
CLASSES = 1000
WL = 128
HL = 32
TOK_IMG = 1024
IMAGES = 8


def place_ends(drawn, own_key, low, high):
    extent = drawn.shape
    spot = [jax.random.randint(jax.random.fold_in(own_key, axis), (), 0, extent[axis]) for axis in range(len(extent))]
    drawn = drawn.at[tuple(spot)].set(low)
    longest = extent.index(max(extent))
    spot[longest] = (spot[longest] + 1) % extent[longest]
    return drawn.at[tuple(spot)].set(high)


def levels(own_key, shape, split, smallest, high):
    def one(position, blocks):
        draws = jax.random.uniform(jax.random.fold_in(jax.random.fold_in(own_key, 6), position), (blocks,), jnp.float32, smallest / len(split), high / len(split))
        return jnp.repeat(jnp.exp(draws), shape[position] // blocks).reshape((-1,) + (1,) * (len(shape) - position - 1))

    factor_of = one(*split[0])
    for cut in split[1:]:
        factor_of = factor_of * one(*cut)
    return factor_of


def centred(key, extent, scale, reach, shards=(), kind=jnp.bfloat16):
    values = scale * jax.random.normal(key, extent, jnp.float32)
    if shards:
        values = values * levels(key, extent, shards, -0.22, 0.18)
    return jnp.clip(values, -reach, reach).astype(kind)


def setup_inputs(seed: int = 0) -> dict:
    keys = jax.random.split(jax.random.key(seed), 10)
    return {
        "feats": centred(keys[0], (IMAGES, HL, WL, C), 1.0, 6.0, ((0, 8), (1, 4))),
        "labels": place_ends(jax.random.randint(keys[1], (IMAGES,), 0, CLASSES), jax.random.fold_in(keys[1], 1), 0, CLASSES - 1).astype(jnp.int32),
        "conv_w": centred(keys[2], (9, C, LAT), (9 * C) ** -0.5, 0.09375),
        "embed_w": centred(keys[3], (4 * LAT, D), (4 * LAT) ** -0.5, 1.5),
        "mod_table": centred(keys[4], (CLASSES, 2 * D), 0.5, 3.0),
        "qkv_w": centred(keys[5], (D, 3 * D), D ** -0.5, 0.1875),
        "out_w": centred(keys[6], (D, D), D ** -0.5, 0.1875),
        "proj_w": centred(keys[7], (D, DINO), D ** -0.5, 0.1875),
        "dino": centred(keys[8], (IMAGES, TOK_IMG, DINO), 1.0, 6.0, ((0, 8), (1, 4))),
    }


latent_scale = 0.18215
norm_eps = 1e-06
cosine_eps = 1e-06

def conv_out(padded, conv_w):
    rows = padded.shape[0] - 2
    cols = padded.shape[1] - 2
    total = jnp.zeros((rows * cols, conv_w.shape[2]), jnp.float32)
    for tap in range(9):
        view = padded[tap // 3:tap // 3 + rows, tap % 3:tap % 3 + cols]
        total = total + jnp.dot(view.reshape(rows * cols, -1), conv_w[tap], preferred_element_type=jnp.float32)
    return total.reshape(rows, cols, -1) * latent_scale

def conv_back(padded, grad_pad, conv_w):
    rows = grad_pad.shape[0] - 2
    cols = grad_pad.shape[1] - 2
    center = grad_pad[1:-1, 1:-1].reshape(rows * cols, -1)
    grad_in = jnp.zeros((rows * cols, conv_w.shape[1]), jnp.float32)
    parts = []
    for tap in range(9):
        row_off = tap // 3
        col_off = tap % 3
        g_view = grad_pad[2 - row_off:2 - row_off + rows, 2 - col_off:2 - col_off + cols].reshape(rows * cols, -1)
        grad_in = grad_in + jnp.dot(g_view, conv_w[tap].T, preferred_element_type=jnp.float32)
        f_view = padded[row_off:row_off + rows, col_off:col_off + cols].reshape(rows * cols, -1)
        parts.append(jnp.dot(f_view.T, center, preferred_element_type=jnp.float32))
    return (grad_in.reshape(rows, cols, -1), jnp.stack(parts, 0))

def patchify(latent):
    rows, cols, chans = latent.shape
    blocks = latent.reshape(rows // 2, 2, cols // 2, 2, chans).transpose(0, 2, 1, 3, 4)
    return blocks.reshape(rows // 2 * (cols // 2), 4 * chans)

def unpatchify(tokens, rows, cols):
    chans = tokens.shape[1] // 4
    blocks = tokens.reshape(rows // 2, cols // 2, 2, 2, chans).transpose(0, 2, 1, 3, 4)
    return blocks.reshape(rows, cols, chans)

def cosine_grad(projected, target):
    norm_p = jnp.sqrt(lax.optimization_barrier(jnp.sum(projected * projected, -1, keepdims=True)) + cosine_eps)
    norm_t = jnp.sqrt(lax.optimization_barrier(jnp.sum(target * target, -1, keepdims=True)) + cosine_eps)
    cosine = lax.optimization_barrier(jnp.sum(projected * target, -1, keepdims=True)) / (norm_p * norm_t)
    grad = cosine * projected / (norm_p * norm_p) - target / (norm_p * norm_t)
    return (cosine[:, 0], grad)

def widen(x):
    return lax.optimization_barrier(x.astype(jnp.bfloat16)).astype(jnp.float32)

def one_image(image, label, target_b, conv_w, embed_w, mod_table, qkv_w, out_w, proj_w):
    rows, cols, chans = image.shape
    width = qkv_w.shape[0]
    heads = width // HEAD_DIM
    scale = HEAD_DIM ** (-0.5)
    padded = jnp.pad(image, ((1, 1), (1, 1), (0, 0)))
    tokens = patchify(conv_out(padded, conv_w))
    count = tokens.shape[0]
    embed_f = embed_w.astype(jnp.float32)
    start = jnp.dot(tokens, embed_f, precision=lax.Precision.HIGHEST)
    row = mod_table[label].astype(jnp.float32)
    mean = lax.optimization_barrier(jnp.mean(start, -1, keepdims=True))
    cent = start - mean
    inv = lax.rsqrt(lax.optimization_barrier(jnp.mean(cent * cent, -1, keepdims=True)) + norm_eps)
    normed = cent * inv
    modded = (normed * (1.0 + row[width:]) + row[:width]).astype(jnp.bfloat16)
    qkv = jnp.dot(modded, qkv_w, preferred_element_type=jnp.float32).astype(jnp.bfloat16)
    q3 = qkv[:, :width].astype(jnp.float32).reshape(count, heads, HEAD_DIM)
    k3 = qkv[:, width:2 * width].astype(jnp.float32).reshape(count, heads, HEAD_DIM)
    v3 = qkv[:, 2 * width:].astype(jnp.float32).reshape(count, heads, HEAD_DIM)
    scores = jnp.einsum('qhd,khd->hqk', q3, k3) * scale
    top = lax.optimization_barrier(jnp.max(scores, -1, keepdims=True))
    expo = jnp.exp(scores - top)
    total = lax.optimization_barrier(jnp.sum(expo, -1))
    attended = jnp.einsum('hqk,khd->qhd', widen(expo), v3) / total.T[:, :, None]
    attended = attended.reshape(count, width).astype(jnp.bfloat16)
    lse = top[..., 0] + jnp.log(total)
    resid = start + jnp.dot(attended, out_w, preferred_element_type=jnp.float32)
    resid_b = resid.astype(jnp.bfloat16)
    projected = jnp.dot(resid_b, proj_w, preferred_element_type=jnp.float32)
    cosine, grad_p = cosine_grad(projected, target_b.astype(jnp.float32))
    grad_pb = grad_p.astype(jnp.bfloat16)
    proj_part = jnp.dot(resid_b.T, grad_pb, preferred_element_type=jnp.float32)
    grad_resid = jnp.dot(grad_pb, proj_w.T, preferred_element_type=jnp.float32)
    grad_att = jnp.dot(grad_resid.astype(jnp.bfloat16), out_w.T, preferred_element_type=jnp.float32).astype(jnp.bfloat16)
    g3 = grad_att.astype(jnp.float32).reshape(count, heads, HEAD_DIM)
    delta = lax.optimization_barrier(jnp.sum(g3 * attended.astype(jnp.float32).reshape(count, heads, HEAD_DIM), -1)).T
    probs = jnp.exp(scores - lse[..., None])
    dprobs = jnp.einsum('qhd,khd->hqk', g3, v3)
    dscores = widen(probs * (dprobs - delta[..., None]))
    grad_q = scale * jnp.einsum('hqk,khd->qhd', dscores, k3).reshape(count, width)
    grad_k = scale * jnp.einsum('hqk,qhd->khd', dscores, q3).reshape(count, width)
    grad_v = jnp.einsum('hqk,qhd->khd', widen(probs), g3).reshape(count, width)
    grad_qkv = jnp.concatenate([grad_q, grad_k, grad_v], 1).astype(jnp.bfloat16)
    grad_mod = jnp.dot(grad_qkv, qkv_w.T, preferred_element_type=jnp.float32)
    grad_norm = grad_mod * (1.0 + row[width:])
    grad_start = grad_resid + inv * (grad_norm - lax.optimization_barrier(jnp.mean(grad_norm, -1, keepdims=True)) - normed * lax.optimization_barrier(jnp.mean(grad_norm * normed, -1, keepdims=True)))
    grad_tokens = jnp.dot(grad_start, embed_f.T, precision=lax.Precision.HIGHEST)
    grad_latent = (unpatchify(grad_tokens, rows, cols) * latent_scale).astype(jnp.bfloat16)
    grad_pad = jnp.pad(grad_latent, ((1, 1), (1, 1), (0, 0)))
    grad_image, conv_part = conv_back(padded, grad_pad, conv_w)
    return (grad_image.astype(jnp.bfloat16), proj_part, conv_part, jnp.sum(1.0 - cosine))

def reference(feats, labels, conv_w, embed_w, mod_table, qkv_w, out_w, proj_w, dino):

    def step(args):
        image, label, target = args
        return one_image(image, label, target, conv_w, embed_w, mod_table, qkv_w, out_w, proj_w)
    grads, proj_parts, conv_parts, losses = lax.map(step, (feats, labels, dino))
    loss = jnp.sum(losses) / (IMAGES * TOK_IMG)
    return (grads, lax.optimization_barrier(jnp.sum(proj_parts, 0)), lax.optimization_barrier(jnp.sum(conv_parts, 0)), loss)
```

```python
import functools

import jax
import jax.numpy as jnp
from jax import lax
from jax.experimental import pallas as pl
from jax.experimental.pallas import tpu as pltpu
from jax.sharding import PartitionSpec as P

HEAD_DIM = 64
PAIR = 2 * HEAD_DIM
LANES = 128
TAPS = 48

latent_scale = 0.18215
norm_eps = 1e-06
cosine_eps = 1e-06

MESH_ID = pl.DeviceIdType.MESH
F32 = jnp.float32
BF16 = jnp.bfloat16


def mm(left, right, dims):
    return lax.dot_general(left, right, (dims, ((), ())), preferred_element_type=F32)


def plain(left, right):
    return mm(left, right, ((1,), (0,)))


def contract_first(left, right):
    return mm(left, right, ((0,), (0,)))


def contract_last(left, right):
    return mm(left, right, ((1,), (1,)))


def split2(x):
    high = x.astype(BF16)
    return high, (x - high.astype(F32)).astype(BF16)


def split3(x):
    high = x.astype(BF16)
    rest = x - high.astype(F32)
    mid = rest.astype(BF16)
    return high, mid, (rest - mid.astype(F32)).astype(BF16)


def iota(shape, dim):
    return lax.broadcasted_iota(jnp.int32, shape, dim)


def shifted(x, by):
    lane = iota(x.shape, 1)
    if by > 0:
        return jnp.where(lane == 0, 0.0, pltpu.roll(x, 1, axis=1))
    return jnp.where(lane == LANES - 1, 0.0, pltpu.roll(x, LANES - 1, axis=1))


def step_kernel(
    slabs, images,
    feats_hbm, taps_ref, embed_ref, row_ref, qkv_hbm, out_hbm, proj_hbm, dino_hbm,
    gfeat_ref, gproj_ref, gconv_ref, loss_ref,
    feats, w_own, out_w, proj_w, dino, load_sems,
    taps48, resp_g, terms, terms_all, stack, tokens, emb, xw, tstack, mt, ep,
    inv_s, gct, k_s, v_s, qt, e_s, r_s, attt, att, residb, gzp, gt_aug, gt, ds_s,
    gk_s, gv_s, gqt, yr, spread, spread_all, vs,
    cbuf, crecv, cfull, gp, gp_recv, gp_out, loss_s,
    dino_sems, t_send, t_recv, a_send, a_recv, s_send, s_recv,
    c_send, c_recv, d_send, d_recv, g_send, g_recv, h_send, h_recv, p_sems,
):
    slab = lax.axis_index("slab")
    image = lax.axis_index("img")
    core = lax.rem(slab, 2)
    chip = slab // 2
    partner = {"slab": slab + 1 - 2 * core, "img": image}
    devices = slabs * images
    chips = devices // 2
    me = slab * images + image
    my_chip = chip * images + image
    width = out_w.shape[0]
    half = width // 2
    full = tokens.shape[1]
    block = dino.shape[1]
    own = 2 * block
    npairs = half // PAIR
    f_rows = emb.shape[0]

    def anyone(j):
        return {"slab": j // images, "img": lax.rem(j, images)}

    def same_core(j):
        return {"slab": (j // images) * 2 + core, "img": lax.rem(j, images)}

    def remote(src, dst, send, recv, device):
        return pltpu.make_async_remote_copy(
            src_ref=src, dst_ref=dst, send_sem=send, recv_sem=recv,
            device_id=device, device_id_type=MESH_ID)

    def others(count, self_index, body):
        def run(step, _):
            body(lax.rem(self_index + step, count))
            return 0

        lax.fori_loop(1, count, run, 0)

    loads = [pltpu.make_async_copy(feats_hbm, feats, load_sems.at[0])]
    for j in range(3):
        loads.append(pltpu.make_async_copy(
            qkv_hbm.at[:, pl.ds(pl.multiple_of(j * width + core * half, LANES), half)],
            w_own.at[j], load_sems.at[1 + j]))
    loads.append(pltpu.make_async_copy(proj_hbm, proj_w, load_sems.at[4]))
    loads.append(pltpu.make_async_copy(out_hbm, out_w, load_sems.at[5]))
    loads.append(pltpu.make_async_copy(dino_hbm, dino.at[core], load_sems.at[6]))
    for c in loads:
        c.start()

    barrier = pltpu.get_barrier_semaphore()
    others(devices, me, lambda j: pl.semaphore_signal(
        barrier, inc=1, device_id=anyone(j), device_id_type=MESH_ID))

    vs[...] = jnp.zeros_like(vs)
    for kx in range(3):
        for ky in range(3):
            vs[kx * 16 + ky * 4 : kx * 16 + ky * 4 + 4, : feats.shape[1]] = (
                taps_ref[ky * 3 + kx].astype(F32))
    taps48[...] = vs[:, : feats.shape[1]].astype(BF16)
    for dy in range(2):
        for dx in range(2):
            emb[dx * 8 + dy * 4 : dx * 8 + dy * 4 + 4, :] = (
                embed_ref[dy * 8 + dx * 4 : dy * 8 + dx * 4 + 4, :].astype(F32))

    loads[0].wait()
    resp = contract_last(taps48[...], feats[...])
    rows = resp.shape[1] // LANES
    for r in range(rows):
        cut = slice(r * LANES, (r + 1) * LANES)
        resp_g[r] = resp[16:32, cut] + shifted(resp[0:16, cut], 1) + shifted(resp[32:48, cut], -1)
    tiles = rows // 2 + 2
    for k in range(tiles):
        for dy in range(2):
            h = 2 * (k - 1) + dy
            total = None
            for ky in range(3):
                r = h + ky - 1
                if 0 <= r < rows:
                    part = resp_g[r, ky * 4 : ky * 4 + 4, :]
                    total = part if total is None else total + part
            if total is None:
                total = jnp.zeros((4, LANES), F32)
            terms[k, dy * 4 : dy * 4 + 4, :] = total

    pl.semaphore_wait(barrier, devices - 1)
    t_copies = []
    for d in range(1, slabs):
        peer = lax.rem(slab + d, slabs)
        t_copies.append(remote(
            terms, terms_all.at[slab], t_send.at[d], t_recv.at[d], {"slab": peer, "img": image}))
    for c in t_copies:
        c.start()
    loads[6].wait()
    dino_copy = remote(dino_hbm, dino.at[core], dino_sems.at[0], dino_sems.at[1], partner)
    dino_copy.start()
    terms_all[slab] = terms[...]

    gain = 1.0 + row_ref[1:2, :]
    stack_l = jnp.concatenate(
        [emb[...] * gain, gain, row_ref[0:1, :], jnp.zeros((6, width), F32)], 0)
    parts = jnp.concatenate(split3(stack_l), 0)
    for j in range(3):
        loads[1 + j].wait()
        prod = plain(parts, w_own[j])
        xw[j] = prod[0:24] + prod[24:48] + prod[48:72]
    ebar = jnp.mean(emb[...], 1, keepdims=True)
    ecent = emb[...] - ebar
    gram = lax.dot_general(
        ecent, ecent, (((1,), (1,)), ((), ())), precision=lax.Precision.HIGHEST,
        preferred_element_type=F32)
    loads[4].wait()
    ep[...] = plain(emb[...].astype(BF16), proj_w[...])
    loads[5].wait()
    mt[...] = plain(
        out_w[pl.ds(pl.multiple_of(core * half, 8), half), :], proj_w[...]).astype(BF16)

    for c in t_copies:
        c.wait_recv()

    per = rows // 2
    for i in range(per * slabs):
        p, k = divmod(i, per)
        lat = terms_all[p, k + 1]
        if k == 0 and p > 0:
            lat = lat + terms_all[p - 1, per + 1]
        if k == per - 1 and p < slabs - 1:
            lat = lat + terms_all[p + 1, 0]
        stack[(i // 2) * 8 : (i // 2) * 8 + 8, (i % 2) * LANES : (i % 2 + 1) * LANES] = (
            lat * latent_scale)
    spots = iota((2 * LANES, 2 * LANES), 0)
    dests = iota((2 * LANES, 2 * LANES), 1)
    hit = jnp.logical_and(
        lax.shift_right_logical(spots, 7) == lax.shift_right_logical(dests & 127, 6),
        (spots & 127) == 2 * (dests & 63) + lax.shift_right_logical(dests, 7))
    select = jnp.where(hit, 1.0, 0.0).astype(BF16)
    lines = stack.shape[0]
    moved = plain(jnp.concatenate(split3(stack[...]), 0), select)
    moved = moved[0:lines] + moved[lines : 2 * lines] + moved[2 * lines :]
    for i2 in range(lines // 8):
        for dx in range(2):
            tokens[dx * 8 : dx * 8 + 8, i2 * LANES : (i2 + 1) * LANES] = (
                moved[i2 * 8 : i2 * 8 + 8, dx * LANES : (dx + 1) * LANES])
    tok = tokens[...]
    emb_b = emb[...].astype(BF16)
    tok3 = jnp.concatenate(split3(tok), 0)
    emb3 = jnp.concatenate([emb_b] * 3, 0)
    invs = []
    for b in range(full // 256):
        st = contract_first(emb3, tok3[:, b * 256 : (b + 1) * 256])
        cent = st - jnp.mean(st, 0, keepdims=True)
        invs.append(lax.rsqrt(jnp.mean(cent * cent, 0, keepdims=True) + norm_eps))
    inv = jnp.concatenate(invs, 1)
    inv_s[...] = inv
    tn = tok * inv
    tokens[...] = tn
    gct[...] = lax.dot_general(
        gram, tn, (((1,), (0,)), ((), ())), precision=lax.Precision.HIGHEST,
        preferred_element_type=F32) * (1.0 / width)
    tn_hi, tn_lo = split2(tn)
    ones = jnp.where(iota((16, full), 0) < 2, 1.0, 0.0).astype(BF16)
    tstack[...] = jnp.concatenate([tn_hi, tn_hi, tn_lo, ones], 0)

    def basis(j):
        b = xw[j, 0:16, :] - ebar * xw[j, 16:17, :]
        b_hi, b_lo = split2(b)
        s_hi, s_lo = split2(xw[j, 17:18, :])
        line = iota((16, half), 0)
        bias = jnp.where(line == 0, s_hi.astype(F32), jnp.where(line == 1, s_lo.astype(F32), 0.0))
        return jnp.concatenate([b_hi, b_lo, b_hi, bias.astype(BF16)], 0)

    bk, bv, bq = basis(1), basis(2), basis(0)
    lane = iota((256, PAIR), 1)
    for b in range(full // 256):
        cut = slice(b * 256, (b + 1) * 256)
        ts = tstack[:, cut]
        kk = contract_first(ts, bk)
        vv = contract_first(ts, bv)
        for p in range(npairs):
            k_s[p, cut, :] = kk[:, p * PAIR : (p + 1) * PAIR].astype(BF16)
            vp = vv[:, p * PAIR : (p + 1) * PAIR]
            v_s[2 * p, cut, :] = jnp.where(
                lane < HEAD_DIM, vp, jnp.where(lane < HEAD_DIM + 2, 1.0, 0.0)).astype(BF16)
            v_s[2 * p + 1, cut, :] = jnp.where(
                lane >= HEAD_DIM, vp, jnp.where(lane < 2, 1.0, 0.0)).astype(BF16)
    chip_cut = pl.ds(pl.multiple_of(chip * own, LANES), own)
    qq = contract_first(bq, tstack[:, chip_cut]).astype(BF16) * BF16(HEAD_DIM ** -0.5)
    blank = jnp.zeros((HEAD_DIM, own), BF16)
    for p in range(npairs):
        qt[2 * p] = jnp.concatenate([qq[p * PAIR : p * PAIR + HEAD_DIM], blank], 0)
        qt[2 * p + 1] = jnp.concatenate([blank, qq[p * PAIR + HEAD_DIM : (p + 1) * PAIR]], 0)

    def att_copy(p):
        return remote(att.at[core, p], att.at[core, p], a_send.at[p], a_recv.at[p], partner)

    def forward(p, _):
        for b in range(own // 256):
            cut = slice(b * 256, (b + 1) * 256)
            tops = []
            for h in range(2):
                s = plain(k_s[p], qt[2 * p + h, :, cut])
                e = jnp.exp(s - jnp.max(s, 0, keepdims=True)).astype(BF16)
                e_s[2 * p + h, :, cut] = e
                o = contract_first(v_s[2 * p + h], e)
                at = HEAD_DIM if h == 0 else 0
                r = 1.0 / o[at : at + 1]
                r_s[p, h : h + 1, cut] = r
                tops.append(o[h * HEAD_DIM : (h + 1) * HEAD_DIM] * r)
            o = jnp.concatenate(tops, 0)
            attt[p, :, cut] = o.astype(BF16)
            att[core, p, cut, :] = o.T.astype(BF16)
        att_copy(p).start()
        return 0

    lax.fori_loop(0, npairs, forward, 0)
    dino_copy.wait()
    for p in range(npairs):
        att_copy(p).wait_recv()

    spread[...] = jnp.zeros_like(spread)
    loss_s[...] = jnp.zeros_like(loss_s)
    vs[...] = jnp.zeros_like(vs)
    tstack[0:48, :] = tok3
    ep_parts = jnp.concatenate(split2(ep[...]), 0)

    def middle(b, _):
        line = pl.ds(pl.multiple_of(b * 256, 256), 256)
        piece = pl.ds(pl.multiple_of(chip * own + b * 256, LANES), 256)
        a = jnp.concatenate([att[i, p, line, :] for i in range(2) for p in range(npairs)], 1)
        resid = contract_first(tstack[0:48, piece], emb3) + plain(a, out_w[...])
        rb = resid.astype(BF16)
        residb[line, :] = rb
        zp = plain(rb, proj_w[...])
        d = dino[b].astype(F32)
        norm_p = jnp.sqrt(jnp.sum(zp * zp, -1, keepdims=True) + cosine_eps)
        norm_t = jnp.sqrt(jnp.sum(d * d, -1, keepdims=True) + cosine_eps)
        cos = jnp.sum(zp * d, -1, keepdims=True) / (norm_p * norm_t)
        g = (zp * (cos / (norm_p * norm_p)) - d / (norm_p * norm_t)).astype(BF16)
        gzp[line, :] = g
        loss_s[...] += jnp.sum(1.0 - cos, 0, keepdims=True) * 0.5
        return 0

    lax.fori_loop(0, own // 256, middle, 0)

    rh = residb[:, pl.ds(pl.multiple_of(core * half, LANES), half)]
    gp_part = contract_first(rh, gzp[...]).astype(BF16)
    gp[...] = gp_part.reshape(gp.shape)
    others(chips, my_chip, lambda j: remote(
        gp.at[j], gp_recv.at[my_chip], g_send.at[j], g_recv.at[my_chip], same_core(j)).start())

    gatt = contract_last(mt[...], gzp[...]).astype(BF16)
    yrr = contract_last(ep_parts, gzp[...])
    yr[...] = (yrr[0:f_rows] + yrr[f_rows : 2 * f_rows]) * 0.5
    line16 = iota((16, own), 0)
    for p in range(npairs):
        g = gatt[p * PAIR : (p + 1) * PAIR].astype(F32)
        prod = g * attt[p].astype(F32)
        for h in range(2):
            cut = slice(h * HEAD_DIM, (h + 1) * HEAD_DIM)
            r = r_s[p, h : h + 1, :]
            delta = jnp.sum(prod[cut], 0, keepdims=True) * r
            d_hi, d_lo = split2(-delta)
            gr = (g[cut] * r).astype(BF16)
            extra = jnp.where(
                line16 == 0, d_hi.astype(F32), jnp.where(line16 == 1, d_lo.astype(F32), 0.0))
            fill = jnp.concatenate(
                [extra.astype(BF16), jnp.zeros((HEAD_DIM - 16, own), BF16)], 0)
            gt_aug[2 * p + h] = jnp.concatenate([gr, fill] if h == 0 else [fill, gr], 0)
            gt[2 * p + h] = jnp.concatenate([gr, blank] if h == 0 else [blank, gr], 0)

    def backward(p, _):
        q_pair = jnp.concatenate([qt[2 * p], qt[2 * p + 1]], 1)
        g_pair = jnp.concatenate([gt[2 * p], gt[2 * p + 1]], 1)
        for c in range(full // 256):
            cut = slice(c * 256, (c + 1) * 256)
            dss, es = [], []
            for h in range(2):
                dp = plain(v_s[2 * p + h, cut, :], gt_aug[2 * p + h])
                e = e_s[2 * p + h, cut, :]
                ds = (e.astype(F32) * dp).astype(BF16)
                ds_s[h, cut, :] = ds
                dss.append(ds)
                es.append(e)
            gk_s[p, cut, :] = contract_last(jnp.concatenate(dss, 1), q_pair).astype(BF16)
            gv_s[p, cut, :] = contract_last(jnp.concatenate(es, 1), g_pair).astype(BF16)
        outs = []
        for h in range(2):
            o = contract_first(k_s[p], ds_s[h])
            outs.append(o[h * HEAD_DIM : (h + 1) * HEAD_DIM] * HEAD_DIM ** -0.5)
        gqt[pl.ds(pl.multiple_of(p * PAIR, PAIR), PAIR), :] = jnp.concatenate(outs, 0).astype(BF16)
        return 0

    lax.fori_loop(0, npairs, backward, 0)

    def weights(j):
        return jnp.concatenate(split2(xw[j]), 0)

    inv = inv_s[...]
    tn = tokens[...]
    y = contract_last(weights(1), jnp.concatenate([gk_s[p] for p in range(npairs)], 1))
    y = y + contract_last(weights(2), jnp.concatenate([gv_s[p] for p in range(npairs)], 1))
    y = y[0:24] + y[24:48]
    yq = plain(weights(0), gqt[...])
    yq = yq[0:24] + yq[24:48]

    def back(y, inv, tn, gct):
        yc = y[0:16] - ebar * y[16:17]
        return inv * (yc - gct * jnp.sum(tn * yc, 0, keepdims=True))

    sp = back(y, inv, tn, gct[...])
    sq = back(yq, inv_s[:, chip_cut], tokens[:, chip_cut], gct[:, chip_cut]) + yr[...]
    for t in range(full // LANES):
        spread[t + 1] = sp[:, t * LANES : (t + 1) * LANES]
    for t in range(own // LANES):
        spread[chip * (own // LANES) + t + 1] += sq[:, t * LANES : (t + 1) * LANES]
    strip = block // LANES
    s_copies = []
    for d in range(1, slabs):
        peer = lax.rem(slab + d, slabs)
        s_copies.append(remote(
            spread.at[pl.ds(peer * strip, strip + 2)], spread_all.at[slab],
            s_send.at[d], s_recv.at[d], {"slab": peer, "img": image}))
    for c in s_copies:
        c.start()
    spread_all[slab] = spread[pl.ds(slab * strip, strip + 2)]
    for c in s_copies:
        c.wait_recv()

    cells = []
    for t in range(strip + 2):
        g = spread_all[0, t]
        for p in range(1, slabs):
            g = g + spread_all[p, t]
        g = (g * latent_scale).astype(BF16)
        cells.append(jnp.concatenate([g[0:8], g[8:16]], 1))
    stack[0 : 8 * (strip + 2), :] = contract_last(jnp.concatenate(cells, 0), select)
    for r in range(rows):
        cut = slice(r * LANES, (r + 1) * LANES)
        for ky in range(3):
            h = r + 1 - ky + 4
            t, rest = divmod(h, 4)
            p, dy = divmod(rest, 2)
            vs[16 + ky * 4 : 20 + ky * 4, cut] = stack[
                t * 8 + dy * 4 : t * 8 + dy * 4 + 4, p * LANES : (p + 1) * LANES]
        mid_view = vs[16:32, cut]
        vs[0:16, cut] = shifted(mid_view, -1)
        vs[32:48, cut] = shifted(mid_view, 1)
    views = vs[...].astype(BF16)
    conv_part = plain(views, feats[...])
    cbuf[...] = jnp.zeros_like(cbuf)
    for i in range(TAPS // 8):
        for j in range(4):
            cbuf[i * 4 + j] = conv_part[i * 8 : i * 8 + 8, j * LANES : (j + 1) * LANES]
    cbuf[TAPS // 2] = jnp.broadcast_to(loss_s[...], (8, LANES))
    others(devices, me, lambda j: remote(
        cbuf.at[j], crecv.at[me], c_send.at[j], c_recv.at[me], anyone(j)).start())
    for b in range(rows * LANES // 256):
        cut = slice(b * 256, (b + 1) * 256)
        gfeat_ref[cut, :] = contract_first(views[:, cut], taps48[...]).astype(BF16)

    others(devices, me, lambda j: remote(
        cbuf.at[me], crecv.at[j], c_send.at[j], c_recv.at[j], anyone(j)).wait_recv())
    total = lax.fori_loop(
        1, devices, lambda i, acc: acc + crecv[lax.rem(me + i, devices)], cbuf[me])
    cfull[me] = total
    others(devices, me, lambda j: remote(
        cfull.at[me], cfull.at[me], d_send.at[j], d_recv.at[me], anyone(j)).start())

    others(chips, my_chip, lambda j: remote(
        gp.at[my_chip], gp_recv.at[j], g_send.at[j], g_recv.at[j], same_core(j)).wait_recv())
    gsum = lax.fori_loop(
        1, chips, lambda i, acc: acc + gp_recv[lax.rem(my_chip + i, chips)].astype(F32),
        gp[my_chip].astype(F32))
    gp_out[core, my_chip] = gsum.astype(BF16)
    others(chips, my_chip, lambda j: remote(
        gp_out.at[core, my_chip], gp_out.at[core, my_chip], h_send.at[j], h_recv.at[my_chip],
        same_core(j)).start())
    others(chips, my_chip, lambda j: remote(
        gp_out.at[core, my_chip], gp_out.at[core, j], h_send.at[j], h_recv.at[j],
        same_core(j)).wait_recv())
    last = remote(gp_out.at[core], gp_out.at[core], p_sems.at[0], p_sems.at[1], partner)
    last.start()

    others(devices, me, lambda j: remote(
        cfull.at[me], cfull.at[j], d_send.at[j], d_recv.at[j], anyone(j)).wait_recv())
    for i in range(TAPS // 8):
        for j in range(4):
            vs[i * 8 : i * 8 + 8, j * LANES : (j + 1) * LANES] = cfull[i * 4 + j]
    for kx in range(3):
        for ky in range(3):
            gconv_ref[ky * 3 + kx] = vs[kx * 16 + ky * 4 : kx * 16 + ky * 4 + 4, : 4 * LANES]
    loss_ref[...] = cfull[TAPS // 2, 0:1, 0:1] * (1.0 / (devices * block))
    gproj_ref[core] = gp_out[core].astype(F32).reshape(gproj_ref.shape[1:])
    remote(
        gp_out.at[core], gp_out.at[1 - core], p_sems.at[0], p_sems.at[1], partner).wait_recv()
    gproj_ref[1 - core] = gp_out[1 - core].astype(F32).reshape(gproj_ref.shape[1:])

    for c in t_copies + s_copies + [last]:
        c.wait_send()
    for p in range(npairs):
        att_copy(p).wait_send()
    others(devices, me, lambda j: remote(
        cbuf.at[j], crecv.at[me], c_send.at[j], c_recv.at[me], anyone(j)).wait_send())
    others(devices, me, lambda j: remote(
        cfull.at[me], cfull.at[me], d_send.at[j], d_recv.at[me], anyone(j)).wait_send())
    others(chips, my_chip, lambda j: remote(
        gp.at[j], gp_recv.at[my_chip], g_send.at[j], g_recv.at[my_chip],
        same_core(j)).wait_send())
    others(chips, my_chip, lambda j: remote(
        gp_out.at[core, my_chip], gp_out.at[core, my_chip], h_send.at[j], h_recv.at[my_chip],
        same_core(j)).wait_send())


def local(feats, labels, conv_w, embed_w, mod_table, qkv_w, out_w, proj_w, dino):
    _, rows, cols, chans = feats.shape
    width = qkv_w.shape[0]
    deep = proj_w.shape[1]
    slabs = lax.axis_size("slab")
    images = lax.axis_size("img")
    devices = slabs * images
    chips = devices // 2
    half = width // 2
    block = dino.shape[1]
    own = 2 * block
    full = slabs * block
    heads = half // HEAD_DIM
    pairs = half // PAIR
    features = embed_w.shape[0]
    taps = conv_w.transpose(0, 2, 1)
    row = lax.dynamic_slice_in_dim(mod_table, labels[0], 1, 0).reshape(2, width).astype(F32)
    vmem = pl.BlockSpec(memory_space=pltpu.VMEM)
    hbm = pl.BlockSpec(memory_space=pl.ANY)
    dma = pltpu.SemaphoreType.DMA
    strip = block // LANES
    V = pltpu.VMEM
    scratch = [
        V((rows * cols, chans), BF16), V((3, width, half), BF16), V((width, width), BF16),
        V((width, deep), BF16), V((2, block, deep), BF16), dma((7,)),
        V((TAPS, chans), BF16), V((rows, 16, LANES), F32), V((rows // 2 + 2, 8, LANES), F32),
        V((slabs, rows // 2 + 2, 8, LANES), F32), V((rows * slabs // 4 * 8, 2 * LANES), F32),
        V((features, full), F32), V((features, width), F32), V((3, 24, half), F32),
        V((64, full), BF16), V((half, deep), BF16), V((features, deep), F32),
        V((1, full), F32), V((features, full), F32), V((pairs, full, PAIR), BF16),
        V((heads, full, PAIR), BF16), V((heads, PAIR, own), BF16), V((heads, full, own), BF16),
        V((pairs, 2, own), F32), V((pairs, PAIR, own), BF16), V((2, pairs, own, PAIR), BF16),
        V((own, width), BF16), V((own, deep), BF16), V((heads, PAIR, own), BF16),
        V((heads, PAIR, own), BF16), V((2, full, own), BF16),
        V((pairs, full, PAIR), BF16), V((pairs, full, PAIR), BF16), V((half, own), BF16),
        V((features, own), F32), V((full // LANES + 2, features, LANES), F32),
        V((slabs, strip + 2, features, LANES), F32), V((TAPS, rows * cols), F32),
        V((devices, 8, LANES), F32), V((devices, 8, LANES), F32), V((devices, 8, LANES), F32),
        V((chips, half // chips, deep), BF16), V((chips, half // chips, deep), BF16),
        V((2, chips, half // chips, deep), BF16), V((1, 1), F32),
        dma((2,)), dma((slabs,)), dma((slabs,)), dma((pairs,)), dma((pairs,)),
        dma((slabs,)), dma((slabs,)), dma((devices,)), dma((devices,)), dma((devices,)),
        dma((devices,)), dma((chips,)), dma((chips,)), dma((chips,)), dma((chips,)), dma((2,)),
    ]
    gfeat, gproj, gconv, loss = pl.pallas_call(
        functools.partial(step_kernel, slabs, images),
        out_shape=[
            jax.ShapeDtypeStruct((rows * cols, chans), BF16),
            jax.ShapeDtypeStruct((2, half, deep), F32),
            jax.ShapeDtypeStruct((9, conv_w.shape[2], chans), F32),
            jax.ShapeDtypeStruct((1, 1), F32),
        ],
        in_specs=[hbm, vmem, vmem, vmem, hbm, hbm, hbm, hbm],
        out_specs=[vmem] * 4,
        scratch_shapes=scratch,
        compiler_params=pltpu.CompilerParams(
            collective_id=0, has_side_effects=True, vmem_limit_bytes=60 * 1024 * 1024),
        name="step",
    )(feats.reshape(rows * cols, chans), taps, embed_w, row, qkv_w, out_w, proj_w, dino[0])
    return (
        gfeat.reshape(feats.shape), gproj.reshape(width, deep), gconv.transpose(0, 2, 1),
        loss.reshape(()),
    )


def solution(mesh):
    in_specs = (
        P("img", "slab", None, None),
        P("img"),
        P(),
        P(),
        P(),
        P(),
        P(),
        P(),
        P("img", "slab", None),
    )
    out_specs = (P("img", "slab", None, None), P(), P(), P())
    return jax.shard_map(local, mesh=mesh, in_specs=in_specs, out_specs=out_specs, check_vma=False)
```

```python
import functools

import jax
import jax.numpy as jnp
from jax import lax
from jax.experimental import pallas as pl
from jax.experimental.pallas import tpu as pltpu
from jax.sharding import PartitionSpec as P

HEAD_DIM = 64
PAIR = 2 * HEAD_DIM
LANES = 128
TAPS = 48
GRANT = 60 * 1024 * 1024

latent_scale = 0.18215
norm_eps = 1e-06
cosine_eps = 1e-06

MESH_ID = pl.DeviceIdType.MESH
F32 = jnp.float32
BF16 = jnp.bfloat16


def mm(left, right, dims):
    return lax.dot_general(left, right, (dims, ((), ())), preferred_element_type=F32)


def plain(left, right):
    return mm(left, right, ((1,), (0,)))


def contract_first(left, right):
    return mm(left, right, ((0,), (0,)))


def contract_last(left, right):
    return mm(left, right, ((1,), (1,)))


def split2(x):
    high = x.astype(BF16)
    return high, (x - high.astype(F32)).astype(BF16)


def split3(x):
    high = x.astype(BF16)
    rest = x - high.astype(F32)
    mid = rest.astype(BF16)
    return high, mid, (rest - mid.astype(F32)).astype(BF16)


def iota(shape, dim):
    return lax.broadcasted_iota(jnp.int32, shape, dim)


def shifted(x, by):
    lane = iota(x.shape, 1)
    if by > 0:
        return jnp.where(lane == 0, 0.0, pltpu.roll(x, 1, axis=1))
    return jnp.where(lane == LANES - 1, 0.0, pltpu.roll(x, LANES - 1, axis=1))


def step_kernel(
    slabs, images,
    feats_hbm, taps_hbm, embed_hbm, row_hbm, qkv_hbm, out_hbm, proj_hbm, dino_hbm,
    views_hbm, tapsb_hbm, gp_hbm, gconv_hbm, loss_hbm,
    feats, taps_s, embed_s, row_s, w_own, out_w, proj_w, dino, load_sems,
    taps48, resp_g, terms, terms_all, stack, tokens, emb, xw, tstack, mt, ep,
    inv_s, gct, k_s, v_s, qt, s_s, e_s, r_s, attt, att, residb, gzp, gt_aug, gt, ds_s,
    gk_s, gv_s, gqt, yr, spread, spread_all, vs,
    cbuf, crecv, cfull, gp, r1, h1, r2, h2, r3, gpo, views_s, gconv_s, loss_s, save_sems, gp_sems,
    dino_sems, t_send, t_recv, a_send, a_recv, s_send, s_recv,
    c_send, c_recv, d_send, d_recv, p1_sems, p2_sems, p3_send, p3_recv, a3_send, a3_recv,
    a2_sems, a1_sems, a0_sems,
):
    slab = lax.axis_index("slab")
    image = lax.axis_index("img")
    core = lax.rem(slab, 2)
    chip = slab // 2
    partner = {"slab": slab + 1 - 2 * core, "img": image}
    devices = slabs * images
    me = slab * images + image
    depth = images // 2
    east, north = lax.rem(image, 2), image // 2
    first = chip + core * (east - chip)
    second = east + core * (chip - east)
    hop1 = {"slab": slab + (1 - core) * (2 - 4 * chip), "img": image + core * (1 - 2 * east)}
    hop2 = {"slab": slab + core * (2 - 4 * chip), "img": image + (1 - core) * (1 - 2 * east)}
    width = out_w.shape[0]
    half = width // 2
    full = tokens.shape[1]
    block = dino.shape[1]
    own = 2 * block
    npairs = half // PAIR
    f_rows = emb.shape[0]

    def anyone(j):
        return {"slab": j // images, "img": lax.rem(j, images)}

    def level(j):
        return {"slab": slab, "img": j * 2 + east}

    def remote(src, dst, send, recv, device):
        return pltpu.make_async_remote_copy(
            src_ref=src, dst_ref=dst, send_sem=send, recv_sem=recv,
            device_id=device, device_id_type=MESH_ID)

    def others(count, self_index, body):
        def run(step, _):
            body(lax.rem(self_index + step, count))
            return 0

        lax.fori_loop(1, count, run, 0)

    barrier = pltpu.get_barrier_semaphore()
    loads = [pltpu.make_async_copy(feats_hbm, feats, load_sems.at[0])]
    for j in range(3):
        loads.append(pltpu.make_async_copy(
            qkv_hbm.at[:, pl.ds(pl.multiple_of(j * width + core * half, LANES), half)],
            w_own.at[j], load_sems.at[1 + j]))
    loads.append(pltpu.make_async_copy(proj_hbm, proj_w, load_sems.at[4]))
    loads.append(pltpu.make_async_copy(
        out_hbm.at[pl.ds(pl.multiple_of(core * half, 8), half)],
        out_w.at[pl.ds(pl.multiple_of(core * half, 8), half)], load_sems.at[5]))
    loads.append(pltpu.make_async_copy(dino_hbm, dino.at[core], load_sems.at[6]))
    loads.append(pltpu.make_async_copy(taps_hbm, taps_s, load_sems.at[7]))
    loads.append(pltpu.make_async_copy(embed_hbm, embed_s, load_sems.at[8]))
    loads.append(pltpu.make_async_copy(row_hbm, row_s, load_sems.at[9]))
    loads.append(pltpu.make_async_copy(
        out_hbm.at[pl.ds(pl.multiple_of((1 - core) * half, 8), half)],
        out_w.at[pl.ds(pl.multiple_of((1 - core) * half, 8), half)], load_sems.at[10]))
    for i in (7, 8, 0, 9, 4, 5, 1, 2, 3, 6, 10):
        loads[i].start()

    others(devices, me, lambda j: pl.semaphore_signal(
        barrier, inc=1, device_id=anyone(j), device_id_type=MESH_ID))

    vs[...] = jnp.zeros_like(vs)
    loads[7].wait()
    loads[8].wait()
    for kx in range(3):
        for ky in range(3):
            vs[kx * 16 + ky * 4 : kx * 16 + ky * 4 + 4, : feats.shape[1]] = (
                taps_s[ky * 3 + kx].astype(F32))
    taps48[...] = vs[:, : feats.shape[1]].astype(BF16)
    saves = [pltpu.make_async_copy(taps48, tapsb_hbm, save_sems.at[0])]
    saves[0].start()
    for dy in range(2):
        for dx in range(2):
            emb[dx * 8 + dy * 4 : dx * 8 + dy * 4 + 4, :] = (
                embed_s[dy * 8 + dx * 4 : dy * 8 + dx * 4 + 4, :].astype(F32))

    loads[0].wait()
    resp = contract_last(taps48[...], feats[...])
    rows = resp.shape[1] // LANES
    for r in range(rows):
        cut = slice(r * LANES, (r + 1) * LANES)
        resp_g[r] = resp[16:32, cut] + shifted(resp[0:16, cut], 1) + shifted(resp[32:48, cut], -1)
    tiles = rows // 2 + 2
    for k in range(tiles):
        for dy in range(2):
            h = 2 * (k - 1) + dy
            total = None
            for ky in range(3):
                r = h + ky - 1
                if 0 <= r < rows:
                    part = resp_g[r, ky * 4 : ky * 4 + 4, :]
                    total = part if total is None else total + part
            if total is None:
                total = jnp.zeros((4, LANES), F32)
            terms[k, dy * 4 : dy * 4 + 4, :] = total

    pl.semaphore_wait(barrier, devices - 1)
    t_copies = []
    for d in range(1, slabs):
        peer = lax.rem(slab + d, slabs)
        t_copies.append(remote(
            terms, terms_all.at[slab], t_send.at[d], t_recv.at[d], {"slab": peer, "img": image}))
    for c in t_copies:
        c.start()
    loads[6].wait()
    dino_copy = remote(dino_hbm, dino.at[core], dino_sems.at[0], dino_sems.at[1], partner)
    dino_copy.start()
    terms_all[slab] = terms[...]

    loads[4].wait()
    ep[...] = plain(emb[...].astype(BF16), proj_w[...])
    loads[5].wait()
    mt[...] = plain(
        out_w[pl.ds(pl.multiple_of(core * half, 8), half), :], proj_w[...]).astype(BF16)
    ebar = jnp.mean(emb[...], 1, keepdims=True)
    ecent = emb[...] - ebar
    gram = lax.dot_general(
        ecent, ecent, (((1,), (1,)), ((), ())), precision=lax.Precision.HIGHEST,
        preferred_element_type=F32)
    loads[9].wait()
    row = row_s[...].astype(F32)
    gain = 1.0 + row[:, width:]
    stack_l = jnp.concatenate(
        [emb[...] * gain, gain, row[:, :width], jnp.zeros((6, width), F32)], 0)
    parts = jnp.concatenate(split3(stack_l), 0)
    for j in range(3):
        loads[1 + j].wait()
        prod = plain(parts, w_own[j])
        xw[j] = prod[0:24] + prod[24:48] + prod[48:72]

    for c in t_copies:
        c.wait_recv()

    per = rows // 2
    for i in range(per * slabs):
        p, k = divmod(i, per)
        lat = terms_all[p, k + 1]
        if k == 0 and p > 0:
            lat = lat + terms_all[p - 1, per + 1]
        if k == per - 1 and p < slabs - 1:
            lat = lat + terms_all[p + 1, 0]
        stack[(i // 2) * 8 : (i // 2) * 8 + 8, (i % 2) * LANES : (i % 2 + 1) * LANES] = (
            lat * latent_scale)
    spots = iota((2 * LANES, 2 * LANES), 0)
    dests = iota((2 * LANES, 2 * LANES), 1)
    hit = jnp.logical_and(
        lax.shift_right_logical(spots, 7) == lax.shift_right_logical(dests & 127, 6),
        (spots & 127) == 2 * (dests & 63) + lax.shift_right_logical(dests, 7))
    select = jnp.where(hit, 1.0, 0.0).astype(BF16)
    lines = stack.shape[0]
    moved = plain(jnp.concatenate(split3(stack[...]), 0), select)
    moved = moved[0:lines] + moved[lines : 2 * lines] + moved[2 * lines :]
    for i2 in range(lines // 8):
        for dx in range(2):
            tokens[dx * 8 : dx * 8 + 8, i2 * LANES : (i2 + 1) * LANES] = (
                moved[i2 * 8 : i2 * 8 + 8, dx * LANES : (dx + 1) * LANES])
    tok = tokens[...]
    emb_b = emb[...].astype(BF16)
    tok3 = jnp.concatenate(split3(tok), 0)
    emb3 = jnp.concatenate([emb_b] * 3, 0)
    invs = []
    for b in range(full // 256):
        st = contract_first(emb3, tok3[:, b * 256 : (b + 1) * 256])
        cent = st - jnp.mean(st, 0, keepdims=True)
        invs.append(lax.rsqrt(jnp.mean(cent * cent, 0, keepdims=True) + norm_eps))
    inv = jnp.concatenate(invs, 1)
    inv_s[...] = inv
    tn = tok * inv
    tokens[...] = tn
    gct[...] = lax.dot_general(
        gram, tn, (((1,), (0,)), ((), ())), precision=lax.Precision.HIGHEST,
        preferred_element_type=F32) * (1.0 / width)
    tn_hi, tn_lo = split2(tn)
    ones = jnp.where(iota((16, full), 0) < 2, 1.0, 0.0).astype(BF16)
    tstack[...] = jnp.concatenate([tn_hi, tn_hi, tn_lo, ones], 0)

    def basis(j):
        b = xw[j, 0:16, :] - ebar * xw[j, 16:17, :]
        b_hi, b_lo = split2(b)
        s_hi, s_lo = split2(xw[j, 17:18, :])
        line = iota((16, half), 0)
        bias = jnp.where(line == 0, s_hi.astype(F32), jnp.where(line == 1, s_lo.astype(F32), 0.0))
        return jnp.concatenate([b_hi, b_lo, b_hi, bias.astype(BF16)], 0)

    bk, bv, bq = basis(1), basis(2), basis(0)
    lane = iota((256, PAIR), 1)
    for b in range(full // 256):
        cut = slice(b * 256, (b + 1) * 256)
        ts = tstack[:, cut]
        kk = contract_first(ts, bk)
        vv = contract_first(ts, bv)
        for p in range(npairs):
            k_s[p, cut, :] = kk[:, p * PAIR : (p + 1) * PAIR].astype(BF16)
            vp = vv[:, p * PAIR : (p + 1) * PAIR]
            v_s[2 * p, cut, :] = jnp.where(
                lane < HEAD_DIM, vp, jnp.where(lane < HEAD_DIM + 2, 1.0, 0.0)).astype(BF16)
            v_s[2 * p + 1, cut, :] = jnp.where(
                lane >= HEAD_DIM, vp, jnp.where(lane < 2, 1.0, 0.0)).astype(BF16)
    chip_cut = pl.ds(pl.multiple_of(chip * own, LANES), own)
    qq = contract_first(bq, tstack[:, chip_cut]).astype(BF16) * BF16(HEAD_DIM ** -0.5)
    blank = jnp.zeros((HEAD_DIM, own), BF16)
    for p in range(npairs):
        qt[2 * p] = jnp.concatenate([qq[p * PAIR : p * PAIR + HEAD_DIM], blank], 0)
        qt[2 * p + 1] = jnp.concatenate([blank, qq[p * PAIR + HEAD_DIM : (p + 1) * PAIR]], 0)

    def att_copy(p):
        return remote(att.at[core, p], att.at[core, p], a_send.at[p], a_recv.at[p], partner)

    units = [(p, b, h) for p in range(npairs) for b in range(own // 256) for h in range(2)]

    def scores(i):
        p, b, h = units[i]
        s = plain(k_s[p], qt[2 * p + h, :, b * 256 : (b + 1) * 256])
        s_s[i % 3] = s
        return jnp.max(s, 0, keepdims=True)

    def weigh(i, top):
        p, b, h = units[i]
        e_s[2 * p + h, :, b * 256 : (b + 1) * 256] = jnp.exp(s_s[i % 3] - top).astype(BF16)

    def gather(i, kept):
        p, b, h = units[i]
        cut = slice(b * 256, (b + 1) * 256)
        o = contract_first(v_s[2 * p + h], e_s[2 * p + h, :, cut])
        at = HEAD_DIM if h == 0 else 0
        r = 1.0 / o[at : at + 1]
        r_s[p, h : h + 1, cut] = r
        kept[h] = o[h * HEAD_DIM : (h + 1) * HEAD_DIM] * r
        if h == 1:
            both = jnp.concatenate(kept, 0)
            attt[p, :, cut] = both.astype(BF16)
            att[core, p, cut, :] = both.T.astype(BF16)
            if b == own // 256 - 1:
                att_copy(p).start()

    kept, top = [None, None], scores(0)
    for i in range(len(units) + 1):
        later = scores(i + 1) if i + 1 < len(units) else None
        if i < len(units):
            weigh(i, top)
        if i > 0:
            gather(i - 1, kept)
        top = later
    loads[10].wait()
    dino_copy.wait()
    for p in range(npairs):
        att_copy(p).wait_recv()

    spread[...] = jnp.zeros_like(spread)
    loss_s[...] = jnp.zeros_like(loss_s)
    vs[...] = jnp.zeros_like(vs)
    tstack[0:48, :] = tok3
    ep_parts = jnp.concatenate(split2(ep[...]), 0)

    def middle(b, _):
        line = pl.ds(pl.multiple_of(b * 256, 256), 256)
        piece = pl.ds(pl.multiple_of(chip * own + b * 256, LANES), 256)
        a = jnp.concatenate([att[i, p, line, :] for i in range(2) for p in range(npairs)], 1)
        resid = contract_first(tstack[0:48, piece], emb3) + plain(a, out_w[...])
        rb = resid.astype(BF16)
        residb[line, :] = rb
        zp = plain(rb, proj_w[...])
        d = dino[b].astype(F32)
        norm_p = jnp.sqrt(jnp.sum(zp * zp, -1, keepdims=True) + cosine_eps)
        norm_t = jnp.sqrt(jnp.sum(d * d, -1, keepdims=True) + cosine_eps)
        cos = jnp.sum(zp * d, -1, keepdims=True) / (norm_p * norm_t)
        g = (zp * (cos / (norm_p * norm_p)) - d / (norm_p * norm_t)).astype(BF16)
        gzp[line, :] = g
        loss_s[...] += jnp.sum(1.0 - cos, 0, keepdims=True) * 0.5
        return 0

    lax.fori_loop(0, own // 256, middle, 0)

    rh = residb[:, pl.ds(pl.multiple_of(core * half, LANES), half)]
    chunks, wide = gp.shape[0], gp.shape[-1]
    ranks = range(chunks)

    def p1(k):
        return remote(gp.at[k, 1 - first], r1.at[k], p1_sems.at[0, k], p1_sems.at[1, k], hop1)

    def p2(k):
        return remote(h1.at[k, 1 - second], r2.at[k], p2_sems.at[0, k], p2_sems.at[1, k], hop2)

    def p3(k, j, slot, sem):
        return remote(h2.at[k, j], r3.at[k, slot], p3_send.at[k, j], p3_recv.at[k, sem], level(j))

    def a3(k, j, slot):
        return remote(
            gpo.at[core, k, first, second, north], gpo.at[core, k, first, second, slot],
            a3_send.at[k, j], a3_recv.at[k, slot], level(j))

    def a2(k, there):
        return remote(
            gpo.at[core, k, first, second], gpo.at[core, k, first, there],
            a2_sems.at[0, k], a2_sems.at[1, k], hop2)

    def a1(k, there):
        return remote(
            gpo.at[core, k, first], gpo.at[core, k, there],
            a1_sems.at[0, k], a1_sems.at[1, k], hop1)

    def a0(k, there):
        return remote(
            gpo.at[core, k], gpo.at[there, k], a0_sems.at[0, k], a0_sems.at[1, k], partner)

    def add1(k):
        p1(k).wait_recv()
        h1[k] = (gp[k, first].astype(F32) + r1[k].astype(F32)).astype(BF16)
        p2(k).start()

    def add2(k):
        p2(k).wait_recv()
        h2[k] = (h1[k, second].astype(F32) + r2[k].astype(F32)).astype(BF16)
        others(depth, north, lambda j: p3(k, j, north, north).start())

    def add3(k):
        others(depth, north, lambda j: p3(k, j, j, j).wait_recv())
        total = lax.fori_loop(
            1, depth, lambda i, acc: acc + r3[k, lax.rem(north + i, depth)].astype(F32),
            h2[k, north].astype(F32))
        gpo[core, k, first, second, north] = total.astype(BF16)
        others(depth, north, lambda j: a3(k, j, north).start())

    def give3(k):
        others(depth, north, lambda j: a3(k, j, j).wait_recv())
        a2(k, second).start()

    def give2(k):
        a2(k, 1 - second).wait_recv()
        a1(k, first).start()

    def give1(k):
        a1(k, 1 - first).wait_recv()
        a0(k, core).start()

    for k in ranks:
        part = contract_first(rh, gzp[:, k * wide : (k + 1) * wide]).astype(BF16)
        gp[k] = part.reshape(gp.shape[1:])
        p1(k).start()

    gatt = contract_last(mt[...], gzp[...]).astype(BF16)
    yrr = contract_last(ep_parts, gzp[...])
    yr[...] = (yrr[0:f_rows] + yrr[f_rows : 2 * f_rows]) * 0.5
    line16 = iota((16, own), 0)
    for p in range(npairs):
        g = gatt[p * PAIR : (p + 1) * PAIR].astype(F32)
        prod = g * attt[p].astype(F32)
        for h in range(2):
            cut = slice(h * HEAD_DIM, (h + 1) * HEAD_DIM)
            r = r_s[p, h : h + 1, :]
            delta = jnp.sum(prod[cut], 0, keepdims=True) * r
            d_hi, d_lo = split2(-delta)
            gr = (g[cut] * r).astype(BF16)
            extra = jnp.where(
                line16 == 0, d_hi.astype(F32), jnp.where(line16 == 1, d_lo.astype(F32), 0.0))
            fill = jnp.concatenate(
                [extra.astype(BF16), jnp.zeros((HEAD_DIM - 16, own), BF16)], 0)
            gt_aug[2 * p + h] = jnp.concatenate([gr, fill] if h == 0 else [fill, gr], 0)
            gt[2 * p + h] = jnp.concatenate([gr, blank] if h == 0 else [blank, gr], 0)

    def backward(p, _):
        q_pair = jnp.concatenate([qt[2 * p], qt[2 * p + 1]], 1)
        g_pair = jnp.concatenate([gt[2 * p], gt[2 * p + 1]], 1)
        for c in range(full // 256):
            cut = slice(c * 256, (c + 1) * 256)
            dss, es = [], []
            for h in range(2):
                dp = plain(v_s[2 * p + h, cut, :], gt_aug[2 * p + h])
                e = e_s[2 * p + h, cut, :]
                ds = (e.astype(F32) * dp).astype(BF16)
                ds_s[h, cut, :] = ds
                dss.append(ds)
                es.append(e)
            gk_s[p, cut, :] = contract_last(jnp.concatenate(dss, 1), q_pair).astype(BF16)
            gv_s[p, cut, :] = contract_last(jnp.concatenate(es, 1), g_pair).astype(BF16)
        outs = []
        for h in range(2):
            o = contract_first(k_s[p], ds_s[h])
            outs.append(o[h * HEAD_DIM : (h + 1) * HEAD_DIM] * HEAD_DIM ** -0.5)
        gqt[pl.ds(pl.multiple_of(p * PAIR, PAIR), PAIR), :] = jnp.concatenate(outs, 0).astype(BF16)
        for k in ranks:
            pl.when(p == min(k + 1, npairs - 1))(functools.partial(add1, k))
        return 0

    lax.fori_loop(0, npairs, backward, 0)

    add2(0)
    def weights(j):
        return jnp.concatenate(split2(xw[j]), 0)

    inv = inv_s[...]
    tn = tokens[...]
    y = contract_last(weights(1), jnp.concatenate([gk_s[p] for p in range(npairs)], 1))
    y = y + contract_last(weights(2), jnp.concatenate([gv_s[p] for p in range(npairs)], 1))
    y = y[0:24] + y[24:48]
    yq = plain(weights(0), gqt[...])
    yq = yq[0:24] + yq[24:48]

    def back(y, inv, tn, gct):
        yc = y[0:16] - ebar * y[16:17]
        return inv * (yc - gct * jnp.sum(tn * yc, 0, keepdims=True))

    sp = back(y, inv, tn, gct[...])
    sq = back(yq, inv_s[:, chip_cut], tokens[:, chip_cut], gct[:, chip_cut]) + yr[...]
    for t in range(full // LANES):
        spread[t + 1] = sp[:, t * LANES : (t + 1) * LANES]
    for t in range(own // LANES):
        spread[chip * (own // LANES) + t + 1] += sq[:, t * LANES : (t + 1) * LANES]
    strip = block // LANES
    s_copies = []
    for d in range(1, slabs):
        peer = lax.rem(slab + d, slabs)
        s_copies.append(remote(
            spread.at[pl.ds(peer * strip, strip + 2)], spread_all.at[slab],
            s_send.at[d], s_recv.at[d], {"slab": peer, "img": image}))
    for c in s_copies:
        c.start()
    spread_all[slab] = spread[pl.ds(slab * strip, strip + 2)]
    for k in ranks[1:]:
        add2(k)
    for c in s_copies:
        c.wait_recv()

    cells = []
    for t in range(strip + 2):
        g = spread_all[0, t]
        for p in range(1, slabs):
            g = g + spread_all[p, t]
        g = (g * latent_scale).astype(BF16)
        cells.append(jnp.concatenate([g[0:8], g[8:16]], 1))
    stack[0 : 8 * (strip + 2), :] = contract_last(jnp.concatenate(cells, 0), select)
    for r in range(rows):
        cut = slice(r * LANES, (r + 1) * LANES)
        for ky in range(3):
            h = r + 1 - ky + 4
            t, rest = divmod(h, 4)
            p, dy = divmod(rest, 2)
            vs[16 + ky * 4 : 20 + ky * 4, cut] = stack[
                t * 8 + dy * 4 : t * 8 + dy * 4 + 4, p * LANES : (p + 1) * LANES]
        mid_view = vs[16:32, cut]
        vs[0:16, cut] = shifted(mid_view, -1)
        vs[32:48, cut] = shifted(mid_view, 1)
    views = vs[...].astype(BF16)
    views_s[...] = views
    saves.append(pltpu.make_async_copy(views_s, views_hbm, save_sems.at[1]))
    saves[-1].start()
    conv_part = plain(views, feats[...])
    cbuf[...] = jnp.zeros_like(cbuf)
    for i in range(TAPS // 8):
        for j in range(4):
            cbuf[i * 4 + j] = conv_part[i * 8 : i * 8 + 8, j * LANES : (j + 1) * LANES]
    cbuf[TAPS // 2] = jnp.broadcast_to(loss_s[...], (8, LANES))
    others(devices, me, lambda j: remote(
        cbuf.at[j], crecv.at[me], c_send.at[j], c_recv.at[me], anyone(j)).start())
    for k in ranks:
        add3(k)
    give3(0)
    others(devices, me, lambda j: remote(
        cbuf.at[me], crecv.at[j], c_send.at[j], c_recv.at[j], anyone(j)).wait_recv())
    total = lax.fori_loop(
        1, devices, lambda i, acc: acc + crecv[lax.rem(me + i, devices)], cbuf[me])
    cfull[me] = total
    others(devices, me, lambda j: remote(
        cfull.at[me], cfull.at[me], d_send.at[j], d_recv.at[me], anyone(j)).start())

    for k in ranks[1:]:
        give3(k)
    for k in ranks:
        give2(k)
    others(devices, me, lambda j: remote(
        cfull.at[me], cfull.at[j], d_send.at[j], d_recv.at[j], anyone(j)).wait_recv())
    for i in range(TAPS // 8):
        for j in range(4):
            vs[i * 8 : i * 8 + 8, j * LANES : (j + 1) * LANES] = cfull[i * 4 + j]
    for kx in range(3):
        for ky in range(3):
            gconv_s[ky * 3 + kx] = vs[kx * 16 + ky * 4 : kx * 16 + ky * 4 + 4, : 4 * LANES]
    loss_s[...] = cfull[TAPS // 2, 0:1, 0:1] * (1.0 / (devices * block))
    saves.append(pltpu.make_async_copy(gconv_s, gconv_hbm, save_sems.at[2]))
    saves.append(pltpu.make_async_copy(loss_s, loss_hbm, save_sems.at[3]))
    for c in saves[-2:]:
        c.start()
    for k in ranks:
        give1(k)
        saves.append(pltpu.make_async_copy(
            gpo.at[core, k], gp_hbm.at[core, k], gp_sems.at[0, k]))
        saves[-1].start()
    for k in ranks:
        a0(k, 1 - core).wait_recv()
        saves.append(pltpu.make_async_copy(
            gpo.at[1 - core, k], gp_hbm.at[1 - core, k], gp_sems.at[1, k]))
        saves[-1].start()
    for c in saves:
        c.wait()

    for c in t_copies + s_copies:
        c.wait_send()
    for p in range(npairs):
        att_copy(p).wait_send()
    others(devices, me, lambda j: remote(
        cbuf.at[j], crecv.at[me], c_send.at[j], c_recv.at[me], anyone(j)).wait_send())
    others(devices, me, lambda j: remote(
        cfull.at[me], cfull.at[me], d_send.at[j], d_recv.at[me], anyone(j)).wait_send())
    for k in ranks:
        p1(k).wait_send()
        p2(k).wait_send()
        others(depth, north, lambda j, k=k: p3(k, j, north, north).wait_send())
        others(depth, north, lambda j, k=k: a3(k, j, north).wait_send())
        a2(k, second).wait_send()
        a1(k, first).wait_send()
        a0(k, core).wait_send()


def finish_kernel(
    views_hbm, taps_hbm, gp_hbm, conv_hbm, sum_hbm, gfeat_hbm, gproj_hbm, gconv_hbm, loss_hbm,
    views, taps, gp, gfeat, gproj, gconv, loss,
    load_sems, gp_sems, sems,
):
    cores, chunks, many, deep, wide = gp.shape
    loads = [
        pltpu.make_async_copy(views_hbm, views, load_sems.at[0]),
        pltpu.make_async_copy(taps_hbm, taps, load_sems.at[1]),
    ]
    parts = [
        pltpu.make_async_copy(gp_hbm.at[i, k], gp.at[i, k], gp_sems.at[i, k])
        for i in range(cores) for k in range(chunks)]
    small = [
        pltpu.make_async_copy(conv_hbm, gconv, load_sems.at[2]),
        pltpu.make_async_copy(sum_hbm, loss, load_sems.at[3]),
    ]
    for c in loads + small + parts:
        c.start()
    for c in loads + small:
        c.wait()
    copies = [
        pltpu.make_async_copy(gconv, gconv_hbm, load_sems.at[4]),
        pltpu.make_async_copy(loss, loss_hbm, load_sems.at[5]),
    ]
    for c in copies:
        c.start()
    lines = gfeat.shape[1]
    for i in range(gfeat.shape[0]):
        gfeat[i] = contract_first(
            views[:, i * lines : (i + 1) * lines], taps[...]).astype(BF16)
        copies.append(pltpu.make_async_copy(
            gfeat.at[i], gfeat_hbm.at[pl.ds(i * lines, lines)], sems.at[0, i]))
        copies[-1].start()
    blocks = gproj.shape[0] // cores
    each = many // blocks
    lines = each * deep
    for i in range(cores * blocks):
        for k in range(chunks):
            if i % blocks == 0:
                parts[i // blocks * chunks + k].wait()
            cut = gp[i // blocks, k, i % blocks * each : (i % blocks + 1) * each]
            gproj[i, :, k * wide : (k + 1) * wide] = cut.astype(F32).reshape(lines, wide)
        copies.append(pltpu.make_async_copy(
            gproj.at[i], gproj_hbm.at[pl.ds(i * lines, lines)], sems.at[1, i]))
        copies[-1].start()
    for c in copies:
        c.wait()


def local(feats, labels, conv_w, embed_w, mod_table, qkv_w, out_w, proj_w, dino):
    _, rows, cols, chans = feats.shape
    width = qkv_w.shape[0]
    deep = proj_w.shape[1]
    slabs = lax.axis_size("slab")
    images = lax.axis_size("img")
    devices = slabs * images
    half = width // 2
    block = dino.shape[1]
    own = 2 * block
    full = slabs * block
    heads = half // HEAD_DIM
    pairs = half // PAIR
    features = embed_w.shape[0]
    taps = conv_w.transpose(0, 2, 1)
    row = lax.dynamic_slice_in_dim(mod_table, labels[0], 1, 0)
    depth = images // 2
    wide = 2 * LANES
    piece = half // (4 * depth)
    chunks = deep // wide
    hbm = pl.BlockSpec(memory_space=pltpu.HBM)
    dma = pltpu.SemaphoreType.DMA
    strip = block // LANES
    V = pltpu.VMEM
    scratch = [
        V((rows * cols, chans), BF16), V(taps.shape, BF16), V(embed_w.shape, BF16),
        V((1, 2 * width), BF16), V((3, width, half), BF16), V((width, width), BF16),
        V((width, deep), BF16), V((2, block, deep), BF16), dma((11,)),
        V((TAPS, chans), BF16), V((rows, 16, LANES), F32), V((rows // 2 + 2, 8, LANES), F32),
        V((slabs, rows // 2 + 2, 8, LANES), F32), V((rows * slabs // 4 * 8, 2 * LANES), F32),
        V((features, full), F32), V((features, width), F32), V((3, 24, half), F32),
        V((64, full), BF16), V((half, deep), BF16), V((features, deep), F32),
        V((1, full), F32), V((features, full), F32), V((pairs, full, PAIR), BF16),
        V((heads, full, PAIR), BF16), V((heads, PAIR, own), BF16), V((3, full, 256), F32),
        V((heads, full, own), BF16),
        V((pairs, 2, own), F32), V((pairs, PAIR, own), BF16), V((2, pairs, own, PAIR), BF16),
        V((own, width), BF16), V((own, deep), BF16), V((heads, PAIR, own), BF16),
        V((heads, PAIR, own), BF16), V((2, full, own), BF16),
        V((pairs, full, PAIR), BF16), V((pairs, full, PAIR), BF16), V((half, own), BF16),
        V((features, own), F32), V((full // LANES + 2, features, LANES), F32),
        V((slabs, strip + 2, features, LANES), F32), V((TAPS, rows * cols), F32),
        V((devices, 8, LANES), F32), V((devices, 8, LANES), F32), V((devices, 8, LANES), F32),
        V((chunks, 2, 2, depth, piece, wide), BF16), V((chunks, 2, depth, piece, wide), BF16),
        V((chunks, 2, depth, piece, wide), BF16), V((chunks, depth, piece, wide), BF16),
        V((chunks, depth, piece, wide), BF16), V((chunks, depth, piece, wide), BF16),
        V((2, chunks, 2, 2, depth, piece, wide), BF16), V((TAPS, rows * cols), BF16),
        V((9, conv_w.shape[2], chans), F32), V((1, 1), F32), dma((4,)), dma((2, chunks)),
        dma((2,)), dma((slabs,)), dma((slabs,)), dma((pairs,)), dma((pairs,)),
        dma((slabs,)), dma((slabs,)), dma((devices,)), dma((devices,)), dma((devices,)),
        dma((devices,)), dma((2, chunks)), dma((2, chunks)), dma((chunks, depth)),
        dma((chunks, depth)), dma((chunks, depth)), dma((chunks, depth)), dma((2, chunks)),
        dma((2, chunks)), dma((2, chunks)),
    ]
    views, tapsb, gp, conv, total = pl.pallas_call(
        functools.partial(step_kernel, slabs, images),
        out_shape=[
            jax.ShapeDtypeStruct((TAPS, rows * cols), BF16),
            jax.ShapeDtypeStruct((TAPS, chans), BF16),
            jax.ShapeDtypeStruct((2, chunks, 2, 2, depth, piece, wide), BF16),
            jax.ShapeDtypeStruct((9, conv_w.shape[2], chans), F32),
            jax.ShapeDtypeStruct((1, 1), F32),
        ],
        in_specs=[hbm] * 8,
        out_specs=[hbm] * 5,
        scratch_shapes=scratch,
        compiler_params=pltpu.CompilerParams(
            collective_id=0, has_side_effects=True, vmem_limit_bytes=GRANT),
        name="step",
    )(feats.reshape(rows * cols, chans), taps, embed_w, row, qkv_w, out_w, proj_w,
      dino[0])
    steps = 4
    gfeat, gproj, gconv, loss = pl.pallas_call(
        finish_kernel,
        in_specs=[hbm] * 5,
        out_specs=[hbm] * 4,
        out_shape=[
            jax.ShapeDtypeStruct((rows * cols, chans), BF16),
            jax.ShapeDtypeStruct((width, deep), F32),
            jax.ShapeDtypeStruct(conv.shape, F32),
            jax.ShapeDtypeStruct((1, 1), F32),
        ],
        scratch_shapes=[
            V((TAPS, rows * cols), BF16), V((TAPS, chans), BF16),
            V((2, chunks, 4 * depth, piece, wide), BF16),
            V((steps, rows * cols // steps, chans), BF16), V((steps, width // steps, deep), F32),
            V(conv.shape, F32), V((1, 1), F32), dma((6,)), dma((2, chunks)), dma((2, steps)),
        ],
        compiler_params=pltpu.CompilerParams(vmem_limit_bytes=GRANT),
        name="finish",
    )(views, tapsb, gp.reshape(2, chunks, 4 * depth, piece, wide), conv, total)
    return (
        gfeat.reshape(feats.shape), gproj.reshape(width, deep), gconv.transpose(0, 2, 1),
        loss.reshape(()),
    )


def solution(mesh):
    in_specs = (
        P("img", "slab", None, None),
        P("img"),
        P(),
        P(),
        P(),
        P(),
        P(),
        P(),
        P("img", "slab", None),
    )
    out_specs = (P("img", "slab", None, None), P(), P(), P())
    return jax.shard_map(local, mesh=mesh, in_specs=in_specs, out_specs=out_specs, check_vma=False)
```

```python
import functools

import jax
import jax.numpy as jnp
from jax import lax
from jax.experimental import pallas as pl
from jax.experimental.pallas import tpu as pltpu
from jax.sharding import PartitionSpec as P

HEAD_DIM = 64
PAIR = 2 * HEAD_DIM
LANES = 128
TAPS = 48
GRANT = 44 * 1024 * 1024

latent_scale = 0.18215
norm_eps = 1e-06
cosine_eps = 1e-06

MESH_ID = pl.DeviceIdType.MESH
F32 = jnp.float32
BF16 = jnp.bfloat16


def mm(left, right, dims):
    return lax.dot_general(left, right, (dims, ((), ())), preferred_element_type=F32)


def plain(left, right):
    return mm(left, right, ((1,), (0,)))


def contract_first(left, right):
    return mm(left, right, ((0,), (0,)))


def contract_last(left, right):
    return mm(left, right, ((1,), (1,)))


def split2(x):
    high = x.astype(BF16)
    return high, (x - high.astype(F32)).astype(BF16)


def split3(x):
    high = x.astype(BF16)
    rest = x - high.astype(F32)
    mid = rest.astype(BF16)
    return high, mid, (rest - mid.astype(F32)).astype(BF16)


def iota(shape, dim):
    return lax.broadcasted_iota(jnp.int32, shape, dim)


def shifted(x, by):
    lane = iota(x.shape, 1)
    if by > 0:
        return jnp.where(lane == 0, 0.0, pltpu.roll(x, 1, axis=1))
    return jnp.where(lane == LANES - 1, 0.0, pltpu.roll(x, LANES - 1, axis=1))


def step_kernel(
    slabs, images,
    feats_hbm, taps_hbm, embed_hbm, row_hbm, qkv_hbm, out_hbm, proj_hbm, dino_hbm,
    gfeat_ref, gproj_ref, gconv_ref, loss_ref,
    feats, taps_s, embed_s, row_s, w_own, out_w, proj_w, dino, load_sems,
    taps48, resp_g, terms, terms_all, stack, tokens, emb, xw, tstack, mt, ep,
    inv_s, gct, k_s, v_s, qt, s_s, e_s, r_s, attt, att, residb, gzp, gt_aug, gt, ds_s,
    gk_s, gv_s, gqt, yr, spread, spread_all, vs,
    cbuf, crecv, cfull, gp, r1, h1, r2, h2, r3, gpo, loss_s,
    dino_sems, t_send, t_recv, a_send, a_recv, s_send, s_recv,
    c_send, c_recv, d_send, d_recv, p1_sems, p2_sems, p3_send, p3_recv, a3_send, a3_recv,
    a2_sems, a1_sems, a0_sems,
):
    slab = lax.axis_index("slab")
    image = lax.axis_index("img")
    core = lax.rem(slab, 2)
    chip = slab // 2
    partner = {"slab": slab + 1 - 2 * core, "img": image}
    devices = slabs * images
    me = slab * images + image
    depth = images // 2
    east, north = lax.rem(image, 2), image // 2
    first = chip + core * (east - chip)
    second = east + core * (chip - east)
    hop1 = {"slab": slab + (1 - core) * (2 - 4 * chip), "img": image + core * (1 - 2 * east)}
    hop2 = {"slab": slab + core * (2 - 4 * chip), "img": image + (1 - core) * (1 - 2 * east)}
    width = out_w.shape[0]
    half = width // 2
    full = tokens.shape[1]
    block = dino.shape[1]
    own = 2 * block
    npairs = half // PAIR
    f_rows = emb.shape[0]

    def anyone(j):
        return {"slab": j // images, "img": lax.rem(j, images)}

    def level(j):
        return {"slab": slab, "img": j * 2 + east}

    def remote(src, dst, send, recv, device):
        return pltpu.make_async_remote_copy(
            src_ref=src, dst_ref=dst, send_sem=send, recv_sem=recv,
            device_id=device, device_id_type=MESH_ID)

    def others(count, self_index, body):
        def run(step, _):
            body(lax.rem(self_index + step, count))
            return 0

        lax.fori_loop(1, count, run, 0)

    barrier = pltpu.get_barrier_semaphore()
    loads = [pltpu.make_async_copy(feats_hbm, feats, load_sems.at[0])]
    for j in range(3):
        loads.append(pltpu.make_async_copy(
            qkv_hbm.at[:, pl.ds(pl.multiple_of(j * width + core * half, LANES), half)],
            w_own.at[j], load_sems.at[1 + j]))
    loads.append(pltpu.make_async_copy(proj_hbm, proj_w, load_sems.at[4]))
    loads.append(pltpu.make_async_copy(
        out_hbm.at[pl.ds(pl.multiple_of(core * half, 8), half)],
        out_w.at[pl.ds(pl.multiple_of(core * half, 8), half)], load_sems.at[5]))
    loads.append(pltpu.make_async_copy(dino_hbm, dino.at[core], load_sems.at[6]))
    loads.append(pltpu.make_async_copy(taps_hbm, taps_s, load_sems.at[7]))
    loads.append(pltpu.make_async_copy(embed_hbm, embed_s, load_sems.at[8]))
    loads.append(pltpu.make_async_copy(row_hbm, row_s, load_sems.at[9]))
    loads.append(pltpu.make_async_copy(
        out_hbm.at[pl.ds(pl.multiple_of((1 - core) * half, 8), half)],
        out_w.at[pl.ds(pl.multiple_of((1 - core) * half, 8), half)], load_sems.at[10]))
    for i in (7, 8, 0, 9, 4, 5, 1, 2, 3, 6, 10):
        loads[i].start()

    others(devices, me, lambda j: pl.semaphore_signal(
        barrier, inc=1, device_id=anyone(j), device_id_type=MESH_ID))

    vs[...] = jnp.zeros_like(vs)
    loads[7].wait()
    loads[8].wait()
    for kx in range(3):
        for ky in range(3):
            vs[kx * 16 + ky * 4 : kx * 16 + ky * 4 + 4, : feats.shape[1]] = (
                taps_s[ky * 3 + kx].astype(F32))
    taps48[...] = vs[:, : feats.shape[1]].astype(BF16)
    for dy in range(2):
        for dx in range(2):
            emb[dx * 8 + dy * 4 : dx * 8 + dy * 4 + 4, :] = (
                embed_s[dy * 8 + dx * 4 : dy * 8 + dx * 4 + 4, :].astype(F32))

    loads[0].wait()
    resp = contract_last(taps48[...], feats[...])
    rows = resp.shape[1] // LANES
    for r in range(rows):
        cut = slice(r * LANES, (r + 1) * LANES)
        resp_g[r] = resp[16:32, cut] + shifted(resp[0:16, cut], 1) + shifted(resp[32:48, cut], -1)
    tiles = rows // 2 + 2
    for k in range(tiles):
        for dy in range(2):
            h = 2 * (k - 1) + dy
            total = None
            for ky in range(3):
                r = h + ky - 1
                if 0 <= r < rows:
                    part = resp_g[r, ky * 4 : ky * 4 + 4, :]
                    total = part if total is None else total + part
            if total is None:
                total = jnp.zeros((4, LANES), F32)
            terms[k, dy * 4 : dy * 4 + 4, :] = total

    pl.semaphore_wait(barrier, devices - 1)
    t_copies = []
    for d in range(1, slabs):
        peer = lax.rem(slab + d, slabs)
        t_copies.append(remote(
            terms, terms_all.at[slab], t_send.at[d], t_recv.at[d], {"slab": peer, "img": image}))
    for c in t_copies:
        c.start()
    loads[6].wait()
    dino_copy = remote(dino_hbm, dino.at[core], dino_sems.at[0], dino_sems.at[1], partner)
    dino_copy.start()
    terms_all[slab] = terms[...]

    loads[4].wait()
    ep[...] = plain(emb[...].astype(BF16), proj_w[...])
    loads[5].wait()
    mt[...] = plain(
        out_w[pl.ds(pl.multiple_of(core * half, 8), half), :], proj_w[...]).astype(BF16)
    ebar = jnp.mean(emb[...], 1, keepdims=True)
    ecent = emb[...] - ebar
    gram = lax.dot_general(
        ecent, ecent, (((1,), (1,)), ((), ())), precision=lax.Precision.HIGHEST,
        preferred_element_type=F32)
    loads[9].wait()
    row = row_s[...]
    gain = 1.0 + row[:, width:]
    stack_l = jnp.concatenate(
        [emb[...] * gain, gain, row[:, :width], jnp.zeros((6, width), F32)], 0)
    parts = jnp.concatenate(split3(stack_l), 0)
    for j in range(3):
        loads[1 + j].wait()
        prod = plain(parts, w_own[j])
        xw[j] = prod[0:24] + prod[24:48] + prod[48:72]

    for c in t_copies:
        c.wait_recv()

    per = rows // 2
    for i in range(per * slabs):
        p, k = divmod(i, per)
        lat = terms_all[p, k + 1]
        if k == 0 and p > 0:
            lat = lat + terms_all[p - 1, per + 1]
        if k == per - 1 and p < slabs - 1:
            lat = lat + terms_all[p + 1, 0]
        stack[(i // 2) * 8 : (i // 2) * 8 + 8, (i % 2) * LANES : (i % 2 + 1) * LANES] = (
            lat * latent_scale)
    spots = iota((2 * LANES, 2 * LANES), 0)
    dests = iota((2 * LANES, 2 * LANES), 1)
    hit = jnp.logical_and(
        lax.shift_right_logical(spots, 7) == lax.shift_right_logical(dests & 127, 6),
        (spots & 127) == 2 * (dests & 63) + lax.shift_right_logical(dests, 7))
    select = jnp.where(hit, 1.0, 0.0).astype(BF16)
    lines = stack.shape[0]
    moved = plain(jnp.concatenate(split3(stack[...]), 0), select)
    moved = moved[0:lines] + moved[lines : 2 * lines] + moved[2 * lines :]
    for i2 in range(lines // 8):
        for dx in range(2):
            tokens[dx * 8 : dx * 8 + 8, i2 * LANES : (i2 + 1) * LANES] = (
                moved[i2 * 8 : i2 * 8 + 8, dx * LANES : (dx + 1) * LANES])
    tok = tokens[...]
    emb_b = emb[...].astype(BF16)
    tok3 = jnp.concatenate(split3(tok), 0)
    emb3 = jnp.concatenate([emb_b] * 3, 0)
    invs = []
    for b in range(full // 256):
        st = contract_first(emb3, tok3[:, b * 256 : (b + 1) * 256])
        cent = st - jnp.mean(st, 0, keepdims=True)
        invs.append(lax.rsqrt(jnp.mean(cent * cent, 0, keepdims=True) + norm_eps))
    inv = jnp.concatenate(invs, 1)
    inv_s[...] = inv
    tn = tok * inv
    tokens[...] = tn
    gct[...] = lax.dot_general(
        gram, tn, (((1,), (0,)), ((), ())), precision=lax.Precision.HIGHEST,
        preferred_element_type=F32) * (1.0 / width)
    tn_hi, tn_lo = split2(tn)
    ones = jnp.where(iota((16, full), 0) < 2, 1.0, 0.0).astype(BF16)
    tstack[...] = jnp.concatenate([tn_hi, tn_hi, tn_lo, ones], 0)

    def basis(j):
        b = xw[j, 0:16, :] - ebar * xw[j, 16:17, :]
        b_hi, b_lo = split2(b)
        s_hi, s_lo = split2(xw[j, 17:18, :])
        line = iota((16, half), 0)
        bias = jnp.where(line == 0, s_hi.astype(F32), jnp.where(line == 1, s_lo.astype(F32), 0.0))
        return jnp.concatenate([b_hi, b_lo, b_hi, bias.astype(BF16)], 0)

    bk, bv, bq = basis(1), basis(2), basis(0)
    lane = iota((256, PAIR), 1)
    for b in range(full // 256):
        cut = slice(b * 256, (b + 1) * 256)
        ts = tstack[:, cut]
        kk = contract_first(ts, bk)
        vv = contract_first(ts, bv)
        for p in range(npairs):
            k_s[p, cut, :] = kk[:, p * PAIR : (p + 1) * PAIR].astype(BF16)
            vp = vv[:, p * PAIR : (p + 1) * PAIR]
            v_s[2 * p, cut, :] = jnp.where(
                lane < HEAD_DIM, vp, jnp.where(lane < HEAD_DIM + 2, 1.0, 0.0)).astype(BF16)
            v_s[2 * p + 1, cut, :] = jnp.where(
                lane >= HEAD_DIM, vp, jnp.where(lane < 2, 1.0, 0.0)).astype(BF16)
    chip_cut = pl.ds(pl.multiple_of(chip * own, LANES), own)
    qq = contract_first(bq, tstack[:, chip_cut]).astype(BF16) * BF16(HEAD_DIM ** -0.5)
    blank = jnp.zeros((HEAD_DIM, own), BF16)
    for p in range(npairs):
        qt[2 * p] = jnp.concatenate([qq[p * PAIR : p * PAIR + HEAD_DIM], blank], 0)
        qt[2 * p + 1] = jnp.concatenate([blank, qq[p * PAIR + HEAD_DIM : (p + 1) * PAIR]], 0)

    def att_copy(p):
        return remote(att.at[core, p], att.at[core, p], a_send.at[p], a_recv.at[p], partner)

    units = [(p, b, h) for p in range(npairs) for b in range(own // 256) for h in range(2)]

    def scores(i):
        p, b, h = units[i]
        s = plain(k_s[p], qt[2 * p + h, :, b * 256 : (b + 1) * 256])
        s_s[i % 3] = s
        return jnp.max(s, 0, keepdims=True)

    def weigh(i, top):
        p, b, h = units[i]
        e_s[2 * p + h, :, b * 256 : (b + 1) * 256] = jnp.exp(s_s[i % 3] - top).astype(BF16)

    def gather(i, kept):
        p, b, h = units[i]
        cut = slice(b * 256, (b + 1) * 256)
        o = contract_first(v_s[2 * p + h], e_s[2 * p + h, :, cut])
        at = HEAD_DIM if h == 0 else 0
        r = 1.0 / o[at : at + 1]
        r_s[p, h : h + 1, cut] = r
        kept[h] = o[h * HEAD_DIM : (h + 1) * HEAD_DIM] * r
        if h == 1:
            both = jnp.concatenate(kept, 0)
            attt[p, :, cut] = both.astype(BF16)
            att[core, p, cut, :] = both.T.astype(BF16)
            if b == own // 256 - 1:
                att_copy(p).start()

    kept, top = [None, None], scores(0)
    for i in range(len(units) + 1):
        later = scores(i + 1) if i + 1 < len(units) else None
        if i < len(units):
            weigh(i, top)
        if i > 0:
            gather(i - 1, kept)
        top = later
    loads[10].wait()
    dino_copy.wait()
    for p in range(npairs):
        att_copy(p).wait_recv()

    spread[...] = jnp.zeros_like(spread)
    loss_s[...] = jnp.zeros_like(loss_s)
    vs[...] = jnp.zeros_like(vs)
    tstack[0:48, :] = tok3
    ep_parts = jnp.concatenate(split2(ep[...]), 0)

    def middle(b, _):
        line = pl.ds(pl.multiple_of(b * 256, 256), 256)
        piece = pl.ds(pl.multiple_of(chip * own + b * 256, LANES), 256)
        a = jnp.concatenate([att[i, p, line, :] for i in range(2) for p in range(npairs)], 1)
        resid = contract_first(tstack[0:48, piece], emb3) + plain(a, out_w[...])
        rb = resid.astype(BF16)
        residb[line, :] = rb
        zp = plain(rb, proj_w[...])
        d = dino[b].astype(F32)
        norm_p = jnp.sqrt(jnp.sum(zp * zp, -1, keepdims=True) + cosine_eps)
        norm_t = jnp.sqrt(jnp.sum(d * d, -1, keepdims=True) + cosine_eps)
        cos = jnp.sum(zp * d, -1, keepdims=True) / (norm_p * norm_t)
        g = (zp * (cos / (norm_p * norm_p)) - d / (norm_p * norm_t)).astype(BF16)
        gzp[line, :] = g
        loss_s[...] += jnp.sum(1.0 - cos, 0, keepdims=True) * 0.5
        return 0

    lax.fori_loop(0, own // 256, middle, 0)

    rh = residb[:, pl.ds(pl.multiple_of(core * half, LANES), half)]
    chunks, wide = gp.shape[0], gp.shape[-1]
    ranks = range(chunks)

    def p1(k):
        return remote(gp.at[k, 1 - first], r1.at[k], p1_sems.at[0, k], p1_sems.at[1, k], hop1)

    def p2(k):
        return remote(h1.at[k, 1 - second], r2.at[k], p2_sems.at[0, k], p2_sems.at[1, k], hop2)

    def p3(k, j, slot, sem):
        return remote(h2.at[k, j], r3.at[k, slot], p3_send.at[k, j], p3_recv.at[k, sem], level(j))

    def a3(k, j, slot):
        return remote(
            gpo.at[core, k, first, second, north], gpo.at[core, k, first, second, slot],
            a3_send.at[k, j], a3_recv.at[k, slot], level(j))

    def a2(k, there):
        return remote(
            gpo.at[core, k, first, second], gpo.at[core, k, first, there],
            a2_sems.at[0, k], a2_sems.at[1, k], hop2)

    def a1(k, there):
        return remote(
            gpo.at[core, k, first], gpo.at[core, k, there],
            a1_sems.at[0, k], a1_sems.at[1, k], hop1)

    def a0(k, there):
        return remote(
            gpo.at[core, k], gpo.at[there, k], a0_sems.at[0, k], a0_sems.at[1, k], partner)

    def add1(k):
        p1(k).wait_recv()
        h1[k] = (gp[k, first].astype(F32) + r1[k].astype(F32)).astype(BF16)
        p2(k).start()

    def add2(k):
        p2(k).wait_recv()
        h2[k] = (h1[k, second].astype(F32) + r2[k].astype(F32)).astype(BF16)
        others(depth, north, lambda j: p3(k, j, north, north).start())

    def add3(k):
        others(depth, north, lambda j: p3(k, j, j, j).wait_recv())
        total = lax.fori_loop(
            1, depth, lambda i, acc: acc + r3[k, lax.rem(north + i, depth)].astype(F32),
            h2[k, north].astype(F32))
        gpo[core, k, first, second, north] = total.astype(BF16)
        others(depth, north, lambda j: a3(k, j, north).start())

    def give3(k):
        others(depth, north, lambda j: a3(k, j, j).wait_recv())
        a2(k, second).start()

    def give2(k):
        a2(k, 1 - second).wait_recv()
        a1(k, first).start()

    def give1(k):
        a1(k, 1 - first).wait_recv()
        a0(k, core).start()

    for k in ranks:
        part = contract_first(rh, gzp[:, k * wide : (k + 1) * wide]).astype(BF16)
        gp[k] = part.reshape(gp.shape[1:])
        p1(k).start()

    gatt = contract_last(mt[...], gzp[...]).astype(BF16)
    yrr = contract_last(ep_parts, gzp[...])
    yr[...] = (yrr[0:f_rows] + yrr[f_rows : 2 * f_rows]) * 0.5
    line16 = iota((16, own), 0)
    for p in range(npairs):
        g = gatt[p * PAIR : (p + 1) * PAIR].astype(F32)
        prod = g * attt[p].astype(F32)
        for h in range(2):
            cut = slice(h * HEAD_DIM, (h + 1) * HEAD_DIM)
            r = r_s[p, h : h + 1, :]
            delta = jnp.sum(prod[cut], 0, keepdims=True) * r
            d_hi, d_lo = split2(-delta)
            gr = (g[cut] * r).astype(BF16)
            extra = jnp.where(
                line16 == 0, d_hi.astype(F32), jnp.where(line16 == 1, d_lo.astype(F32), 0.0))
            fill = jnp.concatenate(
                [extra.astype(BF16), jnp.zeros((HEAD_DIM - 16, own), BF16)], 0)
            gt_aug[2 * p + h] = jnp.concatenate([gr, fill] if h == 0 else [fill, gr], 0)
            gt[2 * p + h] = jnp.concatenate([gr, blank] if h == 0 else [blank, gr], 0)

    def backward(p, _):
        q_pair = jnp.concatenate([qt[2 * p], qt[2 * p + 1]], 1)
        g_pair = jnp.concatenate([gt[2 * p], gt[2 * p + 1]], 1)
        for c in range(full // 256):
            cut = slice(c * 256, (c + 1) * 256)
            dss, es = [], []
            for h in range(2):
                dp = plain(v_s[2 * p + h, cut, :], gt_aug[2 * p + h])
                e = e_s[2 * p + h, cut, :]
                ds = (e.astype(F32) * dp).astype(BF16)
                ds_s[h, cut, :] = ds
                dss.append(ds)
                es.append(e)
            gk_s[p, cut, :] = contract_last(jnp.concatenate(dss, 1), q_pair).astype(BF16)
            gv_s[p, cut, :] = contract_last(jnp.concatenate(es, 1), g_pair).astype(BF16)
        outs = []
        for h in range(2):
            o = contract_first(k_s[p], ds_s[h])
            outs.append(o[h * HEAD_DIM : (h + 1) * HEAD_DIM] * HEAD_DIM ** -0.5)
        gqt[pl.ds(pl.multiple_of(p * PAIR, PAIR), PAIR), :] = jnp.concatenate(outs, 0).astype(BF16)
        for k in ranks:
            pl.when(p == k)(functools.partial(add1, k))
        for k in ranks[:2]:
            pl.when(p == k + 2)(functools.partial(add2, k))
        return 0

    lax.fori_loop(0, npairs, backward, 0)

    def weights(j):
        return jnp.concatenate(split2(xw[j]), 0)

    inv = inv_s[...]
    tn = tokens[...]
    y = contract_last(weights(1), jnp.concatenate([gk_s[p] for p in range(npairs)], 1))
    y = y + contract_last(weights(2), jnp.concatenate([gv_s[p] for p in range(npairs)], 1))
    y = y[0:24] + y[24:48]
    yq = plain(weights(0), gqt[...])
    yq = yq[0:24] + yq[24:48]

    def back(y, inv, tn, gct):
        yc = y[0:16] - ebar * y[16:17]
        return inv * (yc - gct * jnp.sum(tn * yc, 0, keepdims=True))

    sp = back(y, inv, tn, gct[...])
    sq = back(yq, inv_s[:, chip_cut], tokens[:, chip_cut], gct[:, chip_cut]) + yr[...]
    for t in range(full // LANES):
        spread[t + 1] = sp[:, t * LANES : (t + 1) * LANES]
    for t in range(own // LANES):
        spread[chip * (own // LANES) + t + 1] += sq[:, t * LANES : (t + 1) * LANES]
    strip = block // LANES
    s_copies = []
    for d in range(1, slabs):
        peer = lax.rem(slab + d, slabs)
        s_copies.append(remote(
            spread.at[pl.ds(peer * strip, strip + 2)], spread_all.at[slab],
            s_send.at[d], s_recv.at[d], {"slab": peer, "img": image}))
    for c in s_copies:
        c.start()
    spread_all[slab] = spread[pl.ds(slab * strip, strip + 2)]
    for k in ranks[2:]:
        add2(k)
    add3(0)
    for c in s_copies:
        c.wait_recv()

    add3(1)
    cells = []
    for t in range(strip + 2):
        g = spread_all[0, t]
        for p in range(1, slabs):
            g = g + spread_all[p, t]
        g = (g * latent_scale).astype(BF16)
        cells.append(jnp.concatenate([g[0:8], g[8:16]], 1))
    stack[0 : 8 * (strip + 2), :] = contract_last(jnp.concatenate(cells, 0), select)
    for r in range(rows):
        cut = slice(r * LANES, (r + 1) * LANES)
        for ky in range(3):
            h = r + 1 - ky + 4
            t, rest = divmod(h, 4)
            p, dy = divmod(rest, 2)
            vs[16 + ky * 4 : 20 + ky * 4, cut] = stack[
                t * 8 + dy * 4 : t * 8 + dy * 4 + 4, p * LANES : (p + 1) * LANES]
        mid_view = vs[16:32, cut]
        vs[0:16, cut] = shifted(mid_view, -1)
        vs[32:48, cut] = shifted(mid_view, 1)
    views = vs[...].astype(BF16)
    conv_part = plain(views, feats[...])
    cbuf[...] = jnp.zeros_like(cbuf)
    for i in range(TAPS // 8):
        for j in range(4):
            cbuf[i * 4 + j] = conv_part[
                i * 8 : i * 8 + 8, j * LANES : (j + 1) * LANES].astype(BF16)
    loss_hi, loss_lo = split2(loss_s[...])
    cbuf[TAPS // 2] = jnp.where(
        iota((8, LANES), 0) == 0, loss_hi.astype(F32), loss_lo.astype(F32)).astype(BF16)
    used = TAPS // 2 + 1

    def owners(body):
        def run(j, _):
            pl.when(j != me)(lambda: body(j))
            return 0

        lax.fori_loop(0, used, run, 0)

    def scatter(j):
        return remote(cbuf.at[j], crecv.at[me], c_send.at[j], c_recv.at[me], anyone(j))

    def share(j):
        return remote(cfull.at[me], cfull.at[me], d_send.at[j], d_recv.at[me], anyone(j))

    owners(lambda j: scatter(j).start())
    for k in ranks[2:]:
        add3(k)
    for i in range(rows * LANES // 256):
        cut = slice(i * 256, (i + 1) * 256)
        gfeat_ref[cut, :] = contract_first(views[:, cut], taps48[...]).astype(BF16)
    for k in ranks[:2]:
        give3(k)

    @pl.when(me < used)
    def _():
        crecv[me] = cbuf[me]
        others(devices, me, lambda j: remote(
            cbuf.at[me], crecv.at[j], c_send.at[me], c_recv.at[j], anyone(j)).wait_recv())
        total = jnp.sum(crecv[...].astype(F32), 0)
        high = total.astype(BF16)
        cfull[me, 0] = high
        cfull[me, 1] = (total - high.astype(F32)).astype(BF16)
        others(devices, me, lambda j: share(j).start())

    give2(0)
    for k in ranks[2:]:
        give3(k)
    for k in ranks[1:]:
        give2(k)
    owners(lambda j: remote(
        cfull.at[j], cfull.at[j], d_send.at[j], d_recv.at[j], anyone(j)).wait_recv())
    for i in range(TAPS // 8):
        for j in range(4):
            tile = cfull[i * 4 + j].astype(F32)
            vs[i * 8 : i * 8 + 8, j * LANES : (j + 1) * LANES] = tile[0] + tile[1]
    for kx in range(3):
        for ky in range(3):
            gconv_ref[ky * 3 + kx] = vs[kx * 16 + ky * 4 : kx * 16 + ky * 4 + 4, : 4 * LANES]
    tile = cfull[TAPS // 2].astype(F32)
    tile = tile[0] + tile[1]
    loss_ref[...] = (tile[0:1, 0:1] + tile[1:2, 0:1]) * (1.0 / (devices * block))

    def store(side, k):
        gproj_ref[side, :, k * wide : (k + 1) * wide] = (
            gpo[side, k].astype(F32).reshape(half, wide))

    for k in ranks:
        give1(k)
        store(core, k)
        if k > 0:
            a0(k - 1, 1 - core).wait_recv()
            store(1 - core, k - 1)
    a0(chunks - 1, 1 - core).wait_recv()
    store(1 - core, chunks - 1)
    for c in t_copies + s_copies:
        c.wait_send()
    for p in range(npairs):
        att_copy(p).wait_send()
    owners(lambda j: scatter(j).wait_send())

    @pl.when(me < used)
    def _():
        others(devices, me, lambda j: share(j).wait_send())

    for k in ranks:
        p1(k).wait_send()
        p2(k).wait_send()
        others(depth, north, lambda j, k=k: p3(k, j, north, north).wait_send())
        others(depth, north, lambda j, k=k: a3(k, j, north).wait_send())
        a2(k, second).wait_send()
        a1(k, first).wait_send()
        a0(k, core).wait_send()


def finish_kernel(*refs):
    count = (len(refs) - 1) // 2
    sems = refs[-1]
    pieces = 4
    copies = []
    for i in range(count):
        left, right = refs[i], refs[count + i]
        cuts = pieces if len(left.shape) == 2 and left.shape[0] > 8 else 1
        lines = left.shape[0] // cuts
        for j in range(cuts):
            copies.append(pltpu.make_async_copy(
                left.at[j * lines : (j + 1) * lines], right.at[j * lines : (j + 1) * lines],
                sems.at[i, j]))
    for c in copies:
        c.start()
    for c in copies:
        c.wait()


def local(feats, labels, conv_w, embed_w, mod_table, qkv_w, out_w, proj_w, dino):
    _, rows, cols, chans = feats.shape
    width = qkv_w.shape[0]
    deep = proj_w.shape[1]
    slabs = lax.axis_size("slab")
    images = lax.axis_size("img")
    devices = slabs * images
    half = width // 2
    block = dino.shape[1]
    own = 2 * block
    full = slabs * block
    heads = half // HEAD_DIM
    pairs = half // PAIR
    features = embed_w.shape[0]
    taps = conv_w.transpose(0, 2, 1)
    row = lax.dynamic_slice_in_dim(mod_table, labels[0], 1, 0).astype(F32)
    depth = images // 2
    wide = 2 * LANES
    piece = half // (4 * depth)
    chunks = deep // wide
    hbm = pl.BlockSpec(memory_space=pltpu.HBM)
    vmem = pl.BlockSpec(memory_space=pltpu.VMEM)
    dma = pltpu.SemaphoreType.DMA
    strip = block // LANES
    V = pltpu.VMEM
    scratch = [
        V((rows * cols, chans), BF16), V(taps.shape, BF16), V(embed_w.shape, BF16),
        V((1, 2 * width), F32), V((3, width, half), BF16), V((width, width), BF16),
        V((width, deep), BF16), V((2, block, deep), BF16), dma((11,)),
        V((TAPS, chans), BF16), V((rows, 16, LANES), F32), V((rows // 2 + 2, 8, LANES), F32),
        V((slabs, rows // 2 + 2, 8, LANES), F32), V((rows * slabs // 4 * 8, 2 * LANES), F32),
        V((features, full), F32), V((features, width), F32), V((3, 24, half), F32),
        V((64, full), BF16), V((half, deep), BF16), V((features, deep), F32),
        V((1, full), F32), V((features, full), F32), V((pairs, full, PAIR), BF16),
        V((heads, full, PAIR), BF16), V((heads, PAIR, own), BF16), V((3, full, 256), F32),
        V((heads, full, own), BF16),
        V((pairs, 2, own), F32), V((pairs, PAIR, own), BF16), V((2, pairs, own, PAIR), BF16),
        V((own, width), BF16), V((own, deep), BF16), V((heads, PAIR, own), BF16),
        V((heads, PAIR, own), BF16), V((2, full, own), BF16),
        V((pairs, full, PAIR), BF16), V((pairs, full, PAIR), BF16), V((half, own), BF16),
        V((features, own), F32), V((full // LANES + 2, features, LANES), F32),
        V((slabs, strip + 2, features, LANES), F32), V((TAPS, rows * cols), F32),
        V((devices, 8, LANES), BF16), V((devices, 8, LANES), BF16), V((devices, 2, 8, LANES), BF16),
        V((chunks, 2, 2, depth, piece, wide), BF16), V((chunks, 2, depth, piece, wide), BF16),
        V((chunks, 2, depth, piece, wide), BF16), V((chunks, depth, piece, wide), BF16),
        V((chunks, depth, piece, wide), BF16), V((chunks, depth, piece, wide), BF16),
        V((2, chunks, 2, 2, depth, piece, wide), BF16), V((1, 1), F32),
        dma((2,)), dma((slabs,)), dma((slabs,)), dma((pairs,)), dma((pairs,)),
        dma((slabs,)), dma((slabs,)), dma((devices,)), dma((devices,)), dma((devices,)),
        dma((devices,)), dma((2, chunks)), dma((2, chunks)), dma((chunks, depth)),
        dma((chunks, depth)), dma((chunks, depth)), dma((chunks, depth)), dma((2, chunks)),
        dma((2, chunks)), dma((2, chunks)),
    ]
    shapes = [
        jax.ShapeDtypeStruct((rows * cols, chans), BF16),
        jax.ShapeDtypeStruct((2, half, deep), F32),
        jax.ShapeDtypeStruct((9, conv_w.shape[2], chans), F32),
        jax.ShapeDtypeStruct((1, 1), F32),
    ]
    given = (feats.reshape(rows * cols, chans), taps, embed_w, row, qkv_w, out_w, proj_w, dino[0])
    made = pl.pallas_call(
        functools.partial(step_kernel, slabs, images),
        out_shape=shapes,
        in_specs=[hbm] * 8,
        out_specs=[vmem] * 4,
        scratch_shapes=scratch,
        compiler_params=pltpu.CompilerParams(
            collective_id=0, has_side_effects=True, vmem_limit_bytes=GRANT),
        name="step",
    )(*[pltpu.with_memory_space_constraint(x, pltpu.HBM) for x in given])
    made = [made[0], made[1].reshape(width, deep), made[2], made[3]]
    gfeat, gproj, gconv, loss = pl.pallas_call(
        finish_kernel,
        in_specs=[vmem] * 4,
        out_specs=[hbm] * 4,
        out_shape=[jax.ShapeDtypeStruct(m.shape, m.dtype) for m in made],
        scratch_shapes=[dma((4, 4))],
        compiler_params=pltpu.CompilerParams(vmem_limit_bytes=8 * 1024 * 1024),
        name="finish",
    )(*made)
    return (
        gfeat.reshape(feats.shape), gproj.reshape(width, deep), gconv.transpose(0, 2, 1),
        loss.reshape(()),
    )


def solution(mesh):
    in_specs = (
        P("img", "slab", None, None),
        P("img"),
        P(),
        P(),
        P(),
        P(),
        P(),
        P(),
        P("img", "slab", None),
    )
    out_specs = (P("img", "slab", None, None), P(), P(), P())
    return jax.shard_map(local, mesh=mesh, in_specs=in_specs, out_specs=out_specs, check_vma=False)
```

```python
import functools

import jax
import jax.numpy as jnp
from jax import lax
from jax.experimental import pallas as pl
from jax.experimental.pallas import tpu as pltpu
from jax.sharding import PartitionSpec as P

HEAD_DIM = 64
PAIR = 2 * HEAD_DIM
LANES = 128
TAPS = 48
GRANT = 44 * 1024 * 1024

latent_scale = 0.18215
norm_eps = 1e-06
cosine_eps = 1e-06

MESH_ID = pl.DeviceIdType.MESH
F32 = jnp.float32
BF16 = jnp.bfloat16


def mm(left, right, dims):
    return lax.dot_general(left, right, (dims, ((), ())), preferred_element_type=F32)


def plain(left, right):
    return mm(left, right, ((1,), (0,)))


def contract_first(left, right):
    return mm(left, right, ((0,), (0,)))


def contract_last(left, right):
    return mm(left, right, ((1,), (1,)))


def split2(x):
    high = x.astype(BF16)
    return high, (x - high.astype(F32)).astype(BF16)


def split3(x):
    high = x.astype(BF16)
    rest = x - high.astype(F32)
    mid = rest.astype(BF16)
    return high, mid, (rest - mid.astype(F32)).astype(BF16)


def iota(shape, dim):
    return lax.broadcasted_iota(jnp.int32, shape, dim)


def shifted(x, by):
    lane = iota(x.shape, 1)
    if by > 0:
        return jnp.where(lane == 0, 0.0, pltpu.roll(x, 1, axis=1))
    return jnp.where(lane == LANES - 1, 0.0, pltpu.roll(x, LANES - 1, axis=1))


def step_kernel(
    slabs, images,
    feats_hbm, taps_hbm, embed_hbm, row_hbm, qkv_hbm, out_hbm, proj_hbm, dino_hbm,
    gfeat_ref, gproj_ref, gconv_ref, loss_ref,
    feats, taps_s, embed_s, row_s, w_own, out_w, proj_w, dino, load_sems,
    taps48, resp_g, terms, terms_all, stack, tokens, emb, xw, tstack, mt, ep,
    inv_s, gct, k_s, v_s, qt, s_s, e_s, r_s, attt, att, residb, gzp, gt_aug, gt, ds_s,
    gk_s, gv_s, gqt, yr, spread, spread_all, vs,
    cbuf, crecv, cfull, gp, r1, h1, r2, h2, r3, gpo, loss_s,
    dino_sems, t_send, t_recv, a_send, a_recv, s_send, s_recv,
    c_send, c_recv, d_send, d_recv, p1_sems, p2_sems, p3_send, p3_recv, a3_send, a3_recv,
    a2_sems, a1_sems, a0_sems,
):
    slab = lax.axis_index("slab")
    image = lax.axis_index("img")
    core = lax.rem(slab, 2)
    chip = slab // 2
    partner = {"slab": slab + 1 - 2 * core, "img": image}
    devices = slabs * images
    me = slab * images + image
    depth = images // 2
    east, north = lax.rem(image, 2), image // 2
    first = chip + core * (east - chip)
    second = east + core * (chip - east)
    hop1 = {"slab": slab + (1 - core) * (2 - 4 * chip), "img": image + core * (1 - 2 * east)}
    hop2 = {"slab": slab + core * (2 - 4 * chip), "img": image + (1 - core) * (1 - 2 * east)}
    width = out_w.shape[0]
    half = width // 2
    full = tokens.shape[1]
    block = dino.shape[1]
    own = 2 * block
    npairs = half // PAIR
    f_rows = emb.shape[0]

    def anyone(j):
        return {"slab": j // images, "img": lax.rem(j, images)}

    def level(j):
        return {"slab": slab, "img": j * 2 + east}

    def remote(src, dst, send, recv, device):
        return pltpu.make_async_remote_copy(
            src_ref=src, dst_ref=dst, send_sem=send, recv_sem=recv,
            device_id=device, device_id_type=MESH_ID)

    def others(count, self_index, body):
        def run(step, _):
            body(lax.rem(self_index + step, count))
            return 0

        lax.fori_loop(1, count, run, 0)

    barrier = pltpu.get_barrier_semaphore()
    loads = [pltpu.make_async_copy(feats_hbm, feats, load_sems.at[0])]
    for j in range(3):
        loads.append(pltpu.make_async_copy(
            qkv_hbm.at[:, pl.ds(pl.multiple_of(j * width + core * half, LANES), half)],
            w_own.at[j], load_sems.at[1 + j]))
    loads.append(pltpu.make_async_copy(proj_hbm, proj_w, load_sems.at[4]))
    loads.append(pltpu.make_async_copy(
        out_hbm.at[pl.ds(pl.multiple_of(core * half, 8), half)],
        out_w.at[pl.ds(pl.multiple_of(core * half, 8), half)], load_sems.at[5]))
    loads.append(pltpu.make_async_copy(dino_hbm, dino.at[core], load_sems.at[6]))
    loads.append(pltpu.make_async_copy(taps_hbm, taps_s, load_sems.at[7]))
    loads.append(pltpu.make_async_copy(embed_hbm, embed_s, load_sems.at[8]))
    loads.append(pltpu.make_async_copy(row_hbm, row_s, load_sems.at[9]))
    loads.append(pltpu.make_async_copy(
        out_hbm.at[pl.ds(pl.multiple_of((1 - core) * half, 8), half)],
        out_w.at[pl.ds(pl.multiple_of((1 - core) * half, 8), half)], load_sems.at[10]))
    for i in (7, 8, 0, 9, 4, 5, 1, 2, 3, 6, 10):
        loads[i].start()

    others(devices, me, lambda j: pl.semaphore_signal(
        barrier, inc=1, device_id=anyone(j), device_id_type=MESH_ID))

    vs[...] = jnp.zeros_like(vs)
    loads[7].wait()
    loads[8].wait()
    for kx in range(3):
        for ky in range(3):
            vs[kx * 16 + ky * 4 : kx * 16 + ky * 4 + 4, : feats.shape[1]] = (
                taps_s[ky * 3 + kx].astype(F32))
    taps48[...] = vs[:, : feats.shape[1]].astype(BF16)
    for dy in range(2):
        for dx in range(2):
            emb[dx * 8 + dy * 4 : dx * 8 + dy * 4 + 4, :] = (
                embed_s[dy * 8 + dx * 4 : dy * 8 + dx * 4 + 4, :].astype(F32))

    loads[0].wait()
    resp = contract_last(taps48[...], feats[...])
    rows = resp.shape[1] // LANES
    for r in range(rows):
        cut = slice(r * LANES, (r + 1) * LANES)
        resp_g[r] = resp[16:32, cut] + shifted(resp[0:16, cut], 1) + shifted(resp[32:48, cut], -1)
    tiles = rows // 2 + 2
    for k in range(tiles):
        for dy in range(2):
            h = 2 * (k - 1) + dy
            total = None
            for ky in range(3):
                r = h + ky - 1
                if 0 <= r < rows:
                    part = resp_g[r, ky * 4 : ky * 4 + 4, :]
                    total = part if total is None else total + part
            if total is None:
                total = jnp.zeros((4, LANES), F32)
            terms[k, dy * 4 : dy * 4 + 4, :] = total

    pl.semaphore_wait(barrier, devices - 1)
    t_copies = []
    for d in range(1, slabs):
        peer = lax.rem(slab + d, slabs)
        t_copies.append(remote(
            terms, terms_all.at[slab], t_send, t_recv, {"slab": peer, "img": image}))
    for c in t_copies:
        c.start()
    loads[6].wait()
    dino_copy = remote(dino_hbm, dino.at[core], dino_sems.at[0], dino_sems.at[1], partner)
    dino_copy.start()
    terms_all[slab] = terms[...]

    loads[4].wait()
    ep[...] = plain(emb[...].astype(BF16), proj_w[...])
    loads[5].wait()
    mt[...] = plain(
        out_w[pl.ds(pl.multiple_of(core * half, 8), half), :], proj_w[...]).astype(BF16)
    ebar = jnp.mean(emb[...], 1, keepdims=True)
    ecent = emb[...] - ebar
    gram = lax.dot_general(
        ecent, ecent, (((1,), (1,)), ((), ())), precision=lax.Precision.HIGHEST,
        preferred_element_type=F32)
    loads[9].wait()
    row = row_s[...]
    gain = 1.0 + row[:, width:]
    stack_l = jnp.concatenate(
        [emb[...] * gain, gain, row[:, :width], jnp.zeros((6, width), F32)], 0)
    parts = jnp.concatenate(split3(stack_l), 0)
    for j in range(3):
        loads[1 + j].wait()
        prod = plain(parts, w_own[j])
        xw[j] = prod[0:24] + prod[24:48] + prod[48:72]

    few = slabs - 1
    halo_wait = remote(
        terms_all.at[pl.ds(0, few)], terms_all.at[pl.ds(0, few)], t_send, t_recv, partner)
    halo_wait.wait_recv()

    per = rows // 2
    for i in range(per * slabs):
        p, k = divmod(i, per)
        lat = terms_all[p, k + 1]
        if k == 0 and p > 0:
            lat = lat + terms_all[p - 1, per + 1]
        if k == per - 1 and p < slabs - 1:
            lat = lat + terms_all[p + 1, 0]
        stack[(i // 2) * 8 : (i // 2) * 8 + 8, (i % 2) * LANES : (i % 2 + 1) * LANES] = (
            lat * latent_scale)
    spots = iota((2 * LANES, 2 * LANES), 0)
    dests = iota((2 * LANES, 2 * LANES), 1)
    hit = jnp.logical_and(
        lax.shift_right_logical(spots, 7) == lax.shift_right_logical(dests & 127, 6),
        (spots & 127) == 2 * (dests & 63) + lax.shift_right_logical(dests, 7))
    select = jnp.where(hit, 1.0, 0.0).astype(BF16)
    lines = stack.shape[0]
    moved = plain(jnp.concatenate(split3(stack[...]), 0), select)
    moved = moved[0:lines] + moved[lines : 2 * lines] + moved[2 * lines :]
    for i2 in range(lines // 8):
        for dx in range(2):
            tokens[dx * 8 : dx * 8 + 8, i2 * LANES : (i2 + 1) * LANES] = (
                moved[i2 * 8 : i2 * 8 + 8, dx * LANES : (dx + 1) * LANES])
    tok = tokens[...]
    emb_b = emb[...].astype(BF16)
    tok3 = jnp.concatenate(split3(tok), 0)
    emb3 = jnp.concatenate([emb_b] * 3, 0)
    invs = []
    for b in range(full // 256):
        st = contract_first(emb3, tok3[:, b * 256 : (b + 1) * 256])
        cent = st - jnp.mean(st, 0, keepdims=True)
        invs.append(lax.rsqrt(jnp.mean(cent * cent, 0, keepdims=True) + norm_eps))
    inv = jnp.concatenate(invs, 1)
    inv_s[...] = inv
    tn = tok * inv
    tokens[...] = tn
    gct[...] = lax.dot_general(
        gram, tn, (((1,), (0,)), ((), ())), precision=lax.Precision.HIGHEST,
        preferred_element_type=F32) * (1.0 / width)
    tn_hi, tn_lo = split2(tn)
    ones = jnp.where(iota((16, full), 0) < 2, 1.0, 0.0).astype(BF16)
    tstack[...] = jnp.concatenate([tn_hi, tn_hi, tn_lo, ones], 0)

    def basis(j):
        b = xw[j, 0:16, :] - ebar * xw[j, 16:17, :]
        b_hi, b_lo = split2(b)
        s_hi, s_lo = split2(xw[j, 17:18, :])
        line = iota((16, half), 0)
        bias = jnp.where(line == 0, s_hi.astype(F32), jnp.where(line == 1, s_lo.astype(F32), 0.0))
        return jnp.concatenate([b_hi, b_lo, b_hi, bias.astype(BF16)], 0)

    bk, bv, bq = basis(1), basis(2), basis(0)
    lane = iota((256, PAIR), 1)
    for b in range(full // 256):
        cut = slice(b * 256, (b + 1) * 256)
        ts = tstack[:, cut]
        kk = contract_first(ts, bk)
        vv = contract_first(ts, bv)
        for p in range(npairs):
            k_s[p, cut, :] = kk[:, p * PAIR : (p + 1) * PAIR].astype(BF16)
            vp = vv[:, p * PAIR : (p + 1) * PAIR]
            v_s[2 * p, cut, :] = jnp.where(
                lane < HEAD_DIM, vp, jnp.where(lane < HEAD_DIM + 2, 1.0, 0.0)).astype(BF16)
            v_s[2 * p + 1, cut, :] = jnp.where(
                lane >= HEAD_DIM, vp, jnp.where(lane < 2, 1.0, 0.0)).astype(BF16)
    chip_cut = pl.ds(pl.multiple_of(chip * own, LANES), own)
    qq = contract_first(bq, tstack[:, chip_cut]).astype(BF16) * BF16(HEAD_DIM ** -0.5)
    blank = jnp.zeros((HEAD_DIM, own), BF16)
    for p in range(npairs):
        qt[2 * p] = jnp.concatenate([qq[p * PAIR : p * PAIR + HEAD_DIM], blank], 0)
        qt[2 * p + 1] = jnp.concatenate([blank, qq[p * PAIR + HEAD_DIM : (p + 1) * PAIR]], 0)

    def att_copy(p):
        return remote(att.at[core, p], att.at[core, p], a_send, a_recv, partner)

    units = [(p, b, h) for p in range(npairs) for b in range(own // 256) for h in range(2)]

    def scores(i):
        p, b, h = units[i]
        s = plain(k_s[p], qt[2 * p + h, :, b * 256 : (b + 1) * 256])
        s_s[i % 3] = s
        return jnp.max(s, 0, keepdims=True)

    def weigh(i, top):
        p, b, h = units[i]
        e_s[2 * p + h, :, b * 256 : (b + 1) * 256] = jnp.exp(s_s[i % 3] - top).astype(BF16)

    def gather(i, kept):
        p, b, h = units[i]
        cut = slice(b * 256, (b + 1) * 256)
        o = contract_first(v_s[2 * p + h], e_s[2 * p + h, :, cut])
        at = HEAD_DIM if h == 0 else 0
        r = 1.0 / o[at : at + 1]
        r_s[p, h : h + 1, cut] = r
        kept[h] = o[h * HEAD_DIM : (h + 1) * HEAD_DIM] * r
        if h == 1:
            both = jnp.concatenate(kept, 0)
            attt[p, :, cut] = both.astype(BF16)
            att[core, p, cut, :] = both.T.astype(BF16)
            if b == own // 256 - 1:
                att_copy(p).start()

    kept, top = [None, None], scores(0)
    for i in range(len(units) + 1):
        later = scores(i + 1) if i + 1 < len(units) else None
        if i < len(units):
            weigh(i, top)
        if i > 0:
            gather(i - 1, kept)
        top = later
    loads[10].wait()
    dino_copy.wait_recv()
    att_wait = remote(att.at[core], att.at[core], a_send, a_recv, partner)
    att_wait.wait_recv()

    spread[...] = jnp.zeros_like(spread)
    loss_s[...] = jnp.zeros_like(loss_s)
    vs[...] = jnp.zeros_like(vs)
    tstack[0:48, :] = tok3
    ep_parts = jnp.concatenate(split2(ep[...]), 0)

    def middle(b, _):
        line = pl.ds(pl.multiple_of(b * 256, 256), 256)
        piece = pl.ds(pl.multiple_of(chip * own + b * 256, LANES), 256)
        a = jnp.concatenate([att[i, p, line, :] for i in range(2) for p in range(npairs)], 1)
        resid = contract_first(tstack[0:48, piece], emb3) + plain(a, out_w[...])
        rb = resid.astype(BF16)
        residb[line, :] = rb
        zp = plain(rb, proj_w[...])
        d = dino[b].astype(F32)
        norm_p = jnp.sqrt(jnp.sum(zp * zp, -1, keepdims=True) + cosine_eps)
        norm_t = jnp.sqrt(jnp.sum(d * d, -1, keepdims=True) + cosine_eps)
        cos = jnp.sum(zp * d, -1, keepdims=True) / (norm_p * norm_t)
        g = (zp * (cos / (norm_p * norm_p)) - d / (norm_p * norm_t)).astype(BF16)
        gzp[line, :] = g
        loss_s[...] += jnp.sum(1.0 - cos, 0, keepdims=True) * 0.5
        return 0

    lax.fori_loop(0, own // 256, middle, 0)

    rh = residb[:, pl.ds(pl.multiple_of(core * half, LANES), half)]
    chunks, wide = gp.shape[0], gp.shape[-1]
    ranks = range(chunks)

    def p1(k):
        return remote(gp.at[k, 1 - first], r1.at[k], p1_sems.at[chunks], p1_sems.at[k], hop1)

    def p2(k):
        return remote(h1.at[k, 1 - second], r2.at[k], p2_sems.at[chunks], p2_sems.at[k], hop2)

    def p3(k, j):
        return remote(h2.at[k, j], r3.at[k, north], p3_send, p3_recv.at[k], level(j))

    def p3_wait(k):
        some = r3.at[k, pl.ds(0, depth - 1)]
        return remote(some, some, p3_send, p3_recv.at[k], partner)

    def a3(k, j):
        mine = gpo.at[core, k, first, second, north]
        return remote(mine, mine, a3_send, a3_recv.at[k], level(j))

    def a3_wait(k):
        some = gpo.at[core, k, first, second, pl.ds(0, depth - 1)]
        return remote(some, some, a3_send, a3_recv.at[k], partner)

    def a2(k, there):
        return remote(
            gpo.at[core, k, first, second], gpo.at[core, k, first, there],
            a2_sems.at[chunks], a2_sems.at[k], hop2)

    def a1(k, there):
        return remote(
            gpo.at[core, k, first], gpo.at[core, k, there],
            a1_sems.at[chunks], a1_sems.at[k], hop1)

    def a0(k, there):
        return remote(
            gpo.at[core, k], gpo.at[there, k], a0_sems.at[chunks], a0_sems.at[k], partner)

    def add1(k):
        p1(k).wait_recv()
        h1[k] = (gp[k, first].astype(F32) + r1[k].astype(F32)).astype(BF16)
        p2(k).start()

    def add2(k):
        p2(k).wait_recv()
        h2[k] = (h1[k, second].astype(F32) + r2[k].astype(F32)).astype(BF16)
        others(depth, north, lambda j: p3(k, j).start())

    def add3(k):
        p3_wait(k).wait_recv()
        total = lax.fori_loop(
            1, depth, lambda i, acc: acc + r3[k, lax.rem(north + i, depth)].astype(F32),
            h2[k, north].astype(F32))
        gpo[core, k, first, second, north] = total.astype(BF16)
        others(depth, north, lambda j: a3(k, j).start())

    def give3(k):
        a3_wait(k).wait_recv()
        a2(k, second).start()

    def give2(k):
        a2(k, 1 - second).wait_recv()
        a1(k, first).start()

    def give1(k):
        a1(k, 1 - first).wait_recv()
        a0(k, core).start()

    for k in ranks:
        part = contract_first(rh, gzp[:, k * wide : (k + 1) * wide]).astype(BF16)
        gp[k] = part.reshape(gp.shape[1:])
        p1(k).start()

    gatt = contract_last(mt[...], gzp[...]).astype(BF16)
    yrr = contract_last(ep_parts, gzp[...])
    yr[...] = (yrr[0:f_rows] + yrr[f_rows : 2 * f_rows]) * 0.5
    line16 = iota((16, own), 0)
    for p in range(npairs):
        g = gatt[p * PAIR : (p + 1) * PAIR].astype(F32)
        prod = g * attt[p].astype(F32)
        for h in range(2):
            cut = slice(h * HEAD_DIM, (h + 1) * HEAD_DIM)
            r = r_s[p, h : h + 1, :]
            delta = jnp.sum(prod[cut], 0, keepdims=True) * r
            d_hi, d_lo = split2(-delta)
            gr = (g[cut] * r).astype(BF16)
            extra = jnp.where(
                line16 == 0, d_hi.astype(F32), jnp.where(line16 == 1, d_lo.astype(F32), 0.0))
            fill = jnp.concatenate(
                [extra.astype(BF16), jnp.zeros((HEAD_DIM - 16, own), BF16)], 0)
            gt_aug[2 * p + h] = jnp.concatenate([gr, fill] if h == 0 else [fill, gr], 0)
            gt[2 * p + h] = jnp.concatenate([gr, blank] if h == 0 else [blank, gr], 0)

    def backward(p, _):
        q_pair = jnp.concatenate([qt[2 * p], qt[2 * p + 1]], 1)
        g_pair = jnp.concatenate([gt[2 * p], gt[2 * p + 1]], 1)
        for c in range(full // 256):
            cut = slice(c * 256, (c + 1) * 256)
            dss, es = [], []
            for h in range(2):
                dp = plain(v_s[2 * p + h, cut, :], gt_aug[2 * p + h])
                e = e_s[2 * p + h, cut, :]
                ds = (e.astype(F32) * dp).astype(BF16)
                ds_s[h, cut, :] = ds
                dss.append(ds)
                es.append(e)
            gk_s[p, cut, :] = contract_last(jnp.concatenate(dss, 1), q_pair).astype(BF16)
            gv_s[p, cut, :] = contract_last(jnp.concatenate(es, 1), g_pair).astype(BF16)
        outs = []
        for h in range(2):
            o = contract_first(k_s[p], ds_s[h])
            outs.append(o[h * HEAD_DIM : (h + 1) * HEAD_DIM] * HEAD_DIM ** -0.5)
        gqt[pl.ds(pl.multiple_of(p * PAIR, PAIR), PAIR), :] = jnp.concatenate(outs, 0).astype(BF16)
        for k in ranks:
            pl.when(p == k)(functools.partial(add1, k))
        for k in ranks[:2]:
            pl.when(p == k + 2)(functools.partial(add2, k))
        return 0

    lax.fori_loop(0, npairs, backward, 0)

    def weights(j):
        return jnp.concatenate(split2(xw[j]), 0)

    inv = inv_s[...]
    tn = tokens[...]
    y = contract_last(weights(1), jnp.concatenate([gk_s[p] for p in range(npairs)], 1))
    y = y + contract_last(weights(2), jnp.concatenate([gv_s[p] for p in range(npairs)], 1))
    y = y[0:24] + y[24:48]
    yq = plain(weights(0), gqt[...])
    yq = yq[0:24] + yq[24:48]

    def back(y, inv, tn, gct):
        yc = y[0:16] - ebar * y[16:17]
        return inv * (yc - gct * jnp.sum(tn * yc, 0, keepdims=True))

    sp = back(y, inv, tn, gct[...])
    sq = back(yq, inv_s[:, chip_cut], tokens[:, chip_cut], gct[:, chip_cut]) + yr[...]
    for t in range(full // LANES):
        spread[t + 1] = sp[:, t * LANES : (t + 1) * LANES]
    for t in range(own // LANES):
        spread[chip * (own // LANES) + t + 1] += sq[:, t * LANES : (t + 1) * LANES]
    strip = block // LANES
    s_copies = []
    for d in range(1, slabs):
        peer = lax.rem(slab + d, slabs)
        s_copies.append(remote(
            spread.at[pl.ds(peer * strip, strip + 2)], spread_all.at[slab],
            s_send, s_recv, {"slab": peer, "img": image}))
    for c in s_copies:
        c.start()
    spread_all[slab] = spread[pl.ds(slab * strip, strip + 2)]
    for k in ranks[2:]:
        add2(k)
    add3(0)
    back_wait = remote(
        spread_all.at[pl.ds(0, few)], spread_all.at[pl.ds(0, few)], s_send, s_recv, partner)
    back_wait.wait_recv()

    add3(1)
    cells = []
    for t in range(strip + 2):
        g = spread_all[0, t]
        for p in range(1, slabs):
            g = g + spread_all[p, t]
        g = (g * latent_scale).astype(BF16)
        cells.append(jnp.concatenate([g[0:8], g[8:16]], 1))
    stack[0 : 8 * (strip + 2), :] = contract_last(jnp.concatenate(cells, 0), select)
    for r in range(rows):
        cut = slice(r * LANES, (r + 1) * LANES)
        for ky in range(3):
            h = r + 1 - ky + 4
            t, rest = divmod(h, 4)
            p, dy = divmod(rest, 2)
            vs[16 + ky * 4 : 20 + ky * 4, cut] = stack[
                t * 8 + dy * 4 : t * 8 + dy * 4 + 4, p * LANES : (p + 1) * LANES]
        mid_view = vs[16:32, cut]
        vs[0:16, cut] = shifted(mid_view, -1)
        vs[32:48, cut] = shifted(mid_view, 1)
    views = vs[...].astype(BF16)
    conv_part = plain(views, feats[...])
    cbuf[...] = jnp.zeros_like(cbuf)
    for i in range(TAPS // 8):
        for j in range(4):
            cbuf[i * 4 + j] = conv_part[
                i * 8 : i * 8 + 8, j * LANES : (j + 1) * LANES].astype(BF16)
    loss_hi, loss_lo = split2(loss_s[...])
    cbuf[TAPS // 2] = jnp.where(
        iota((8, LANES), 0) == 0, loss_hi.astype(F32), loss_lo.astype(F32)).astype(BF16)
    used = TAPS // 2 + 1

    def owners(body):
        def run(j, _):
            pl.when(j != me)(lambda: body(j))
            return 0

        lax.fori_loop(0, used, run, 0)

    def scatter(j):
        return remote(cbuf.at[j], crecv.at[me], c_send, c_recv, anyone(j))

    def tiles_of(ref, count, send, recv):
        return remote(ref.at[pl.ds(0, count)], ref.at[pl.ds(0, count)], send, recv, partner)

    def by_role(body):
        pl.when(me < used)(lambda: body(used - 1))
        pl.when(me >= used)(lambda: body(used))

    def share(j):
        return remote(cfull.at[me], cfull.at[me], d_send, d_recv, anyone(j))

    owners(lambda j: scatter(j).start())
    for k in ranks[2:]:
        add3(k)
    for i in range(rows * LANES // 256):
        cut = slice(i * 256, (i + 1) * 256)
        gfeat_ref[cut, :] = contract_first(views[:, cut], taps48[...]).astype(BF16)
    for k in ranks[:2]:
        give3(k)

    @pl.when(me < used)
    def _():
        crecv[me] = cbuf[me]
        tiles_of(crecv, devices - 1, c_send, c_recv).wait_recv()
        total = jnp.sum(crecv[...].astype(F32), 0)
        high = total.astype(BF16)
        cfull[me, 0] = high
        cfull[me, 1] = (total - high.astype(F32)).astype(BF16)
        others(devices, me, lambda j: share(j).start())

    give2(0)
    for k in ranks[2:]:
        give3(k)
    for k in ranks[1:]:
        give2(k)
    halo_wait.wait_send()
    dino_copy.wait_send()
    att_wait.wait_send()
    back_wait.wait_send()
    by_role(lambda count: tiles_of(cbuf, count, c_send, c_recv).wait_send())
    remote(r1, r1, p1_sems.at[chunks], p1_sems.at[0], partner).wait_send()
    remote(r2, r2, p2_sems.at[chunks], p2_sems.at[0], partner).wait_send()
    every = r3.at[:, pl.ds(0, depth - 1)]
    remote(every, every, p3_send, p3_recv.at[0], partner).wait_send()
    by_role(lambda count: tiles_of(cfull, count, d_send, d_recv).wait_recv())
    for i in range(TAPS // 8):
        for j in range(4):
            tile = cfull[i * 4 + j].astype(F32)
            vs[i * 8 : i * 8 + 8, j * LANES : (j + 1) * LANES] = tile[0] + tile[1]
    for kx in range(3):
        for ky in range(3):
            gconv_ref[ky * 3 + kx] = vs[kx * 16 + ky * 4 : kx * 16 + ky * 4 + 4, : 4 * LANES]
    tile = cfull[TAPS // 2].astype(F32)
    tile = tile[0] + tile[1]
    loss_ref[...] = (tile[0:1, 0:1] + tile[1:2, 0:1]) * (1.0 / (devices * block))

    def store(side, k):
        gproj_ref[side, :, k * wide : (k + 1) * wide] = (
            gpo[side, k].astype(F32).reshape(half, wide))

    for k in ranks:
        give1(k)
        store(core, k)
        if k > 0:
            a0(k - 1, 1 - core).wait_recv()
            store(1 - core, k - 1)
    a0(chunks - 1, 1 - core).wait_recv()
    store(1 - core, chunks - 1)
    @pl.when(me < used)
    def _():
        tiles_of(cfull, devices - 1, d_send, d_recv).wait_send()

    for ref, send, recv in (
        (gpo.at[core, :, first, second, pl.ds(0, depth - 1)], a3_send, a3_recv.at[0]),
        (gpo.at[core, :, first, second], a2_sems.at[chunks], a2_sems.at[0]),
        (gpo.at[core, :, first], a1_sems.at[chunks], a1_sems.at[0]),
        (gpo.at[core], a0_sems.at[chunks], a0_sems.at[0]),
    ):
        remote(ref, ref, send, recv, partner).wait_send()


def finish_kernel(*refs):
    count = (len(refs) - 1) // 2
    sems = refs[-1]
    pieces = 4
    copies = []
    for i in range(count):
        left, right = refs[i], refs[count + i]
        cuts = pieces if len(left.shape) == 2 and left.shape[0] > 8 else 1
        lines = left.shape[0] // cuts
        for j in range(cuts):
            copies.append(pltpu.make_async_copy(
                left.at[j * lines : (j + 1) * lines], right.at[j * lines : (j + 1) * lines],
                sems.at[i, j]))
    for c in copies:
        c.start()
    for c in copies:
        c.wait()


def local(feats, labels, conv_w, embed_w, mod_table, qkv_w, out_w, proj_w, dino):
    _, rows, cols, chans = feats.shape
    width = qkv_w.shape[0]
    deep = proj_w.shape[1]
    slabs = lax.axis_size("slab")
    images = lax.axis_size("img")
    devices = slabs * images
    half = width // 2
    block = dino.shape[1]
    own = 2 * block
    full = slabs * block
    heads = half // HEAD_DIM
    pairs = half // PAIR
    features = embed_w.shape[0]
    taps = conv_w.transpose(0, 2, 1)
    row = lax.dynamic_slice_in_dim(mod_table, labels[0], 1, 0).astype(F32)
    depth = images // 2
    wide = 2 * LANES
    piece = half // (4 * depth)
    chunks = deep // wide
    hbm = pl.BlockSpec(memory_space=pltpu.HBM)
    vmem = pl.BlockSpec(memory_space=pltpu.VMEM)
    dma = pltpu.SemaphoreType.DMA
    strip = block // LANES
    V = pltpu.VMEM
    scratch = [
        V((rows * cols, chans), BF16), V(taps.shape, BF16), V(embed_w.shape, BF16),
        V((1, 2 * width), F32), V((3, width, half), BF16), V((width, width), BF16),
        V((width, deep), BF16), V((2, block, deep), BF16), dma((11,)),
        V((TAPS, chans), BF16), V((rows, 16, LANES), F32), V((rows // 2 + 2, 8, LANES), F32),
        V((slabs, rows // 2 + 2, 8, LANES), F32), V((rows * slabs // 4 * 8, 2 * LANES), F32),
        V((features, full), F32), V((features, width), F32), V((3, 24, half), F32),
        V((64, full), BF16), V((half, deep), BF16), V((features, deep), F32),
        V((1, full), F32), V((features, full), F32), V((pairs, full, PAIR), BF16),
        V((heads, full, PAIR), BF16), V((heads, PAIR, own), BF16), V((3, full, 256), F32),
        V((heads, full, own), BF16),
        V((pairs, 2, own), F32), V((pairs, PAIR, own), BF16), V((2, pairs, own, PAIR), BF16),
        V((own, width), BF16), V((own, deep), BF16), V((heads, PAIR, own), BF16),
        V((heads, PAIR, own), BF16), V((2, full, own), BF16),
        V((pairs, full, PAIR), BF16), V((pairs, full, PAIR), BF16), V((half, own), BF16),
        V((features, own), F32), V((full // LANES + 2, features, LANES), F32),
        V((slabs, strip + 2, features, LANES), F32), V((TAPS, rows * cols), F32),
        V((devices, 8, LANES), BF16), V((devices, 8, LANES), BF16), V((devices, 2, 8, LANES), BF16),
        V((chunks, 2, 2, depth, piece, wide), BF16), V((chunks, 2, depth, piece, wide), BF16),
        V((chunks, 2, depth, piece, wide), BF16), V((chunks, depth, piece, wide), BF16),
        V((chunks, depth, piece, wide), BF16), V((chunks, depth, piece, wide), BF16),
        V((2, chunks, 2, 2, depth, piece, wide), BF16), V((1, 1), F32),
        dma((2,)), dma, dma, dma, dma, dma, dma, dma, dma, dma, dma, dma((chunks + 1,)),
        dma((chunks + 1,)), dma, dma((chunks,)), dma, dma((chunks,)), dma((chunks + 1,)),
        dma((chunks + 1,)), dma((chunks + 1,)),
    ]
    shapes = [
        jax.ShapeDtypeStruct((rows * cols, chans), BF16),
        jax.ShapeDtypeStruct((2, half, deep), F32),
        jax.ShapeDtypeStruct((9, conv_w.shape[2], chans), F32),
        jax.ShapeDtypeStruct((1, 1), F32),
    ]
    given = (feats.reshape(rows * cols, chans), taps, embed_w, row, qkv_w, out_w, proj_w, dino[0])
    made = pl.pallas_call(
        functools.partial(step_kernel, slabs, images),
        out_shape=shapes,
        in_specs=[hbm] * 8,
        out_specs=[vmem] * 4,
        scratch_shapes=scratch,
        compiler_params=pltpu.CompilerParams(
            collective_id=0, has_side_effects=True, vmem_limit_bytes=GRANT),
        name="step",
    )(*[pltpu.with_memory_space_constraint(x, pltpu.HBM) for x in given])
    made = [made[0], made[1].reshape(width, deep), made[2], made[3]]
    gfeat, gproj, gconv, loss = pl.pallas_call(
        finish_kernel,
        in_specs=[vmem] * 4,
        out_specs=[hbm] * 4,
        out_shape=[jax.ShapeDtypeStruct(m.shape, m.dtype) for m in made],
        scratch_shapes=[dma((4, 4))],
        compiler_params=pltpu.CompilerParams(vmem_limit_bytes=8 * 1024 * 1024),
        name="finish",
    )(*made)
    return (
        gfeat.reshape(feats.shape), gproj.reshape(width, deep), gconv.transpose(0, 2, 1),
        loss.reshape(()),
    )


def solution(mesh):
    in_specs = (
        P("img", "slab", None, None),
        P("img"),
        P(),
        P(),
        P(),
        P(),
        P(),
        P(),
        P("img", "slab", None),
    )
    out_specs = (P("img", "slab", None, None), P(), P(), P())
    return jax.shard_map(local, mesh=mesh, in_specs=in_specs, out_specs=out_specs, check_vma=False)
```

```python
import functools

import jax
import jax.numpy as jnp
from jax import lax
from jax.experimental import pallas as pl
from jax.experimental.pallas import tpu as pltpu
from jax.sharding import PartitionSpec as P

HEAD_DIM = 64
PAIR = 2 * HEAD_DIM
LANES = 128
TAPS = 48
GRANT = 44 * 1024 * 1024

latent_scale = 0.18215
norm_eps = 1e-06
cosine_eps = 1e-06

MESH_ID = pl.DeviceIdType.MESH
F32 = jnp.float32
BF16 = jnp.bfloat16


def mm(left, right, dims):
    return lax.dot_general(left, right, (dims, ((), ())), preferred_element_type=F32)


def plain(left, right):
    return mm(left, right, ((1,), (0,)))


def contract_first(left, right):
    return mm(left, right, ((0,), (0,)))


def contract_last(left, right):
    return mm(left, right, ((1,), (1,)))


def split2(x):
    high = x.astype(BF16)
    return high, (x - high.astype(F32)).astype(BF16)


def split3(x):
    high = x.astype(BF16)
    rest = x - high.astype(F32)
    mid = rest.astype(BF16)
    return high, mid, (rest - mid.astype(F32)).astype(BF16)


def iota(shape, dim):
    return lax.broadcasted_iota(jnp.int32, shape, dim)


def shifted(x, by):
    lane = iota(x.shape, 1)
    if by > 0:
        return jnp.where(lane == 0, 0.0, pltpu.roll(x, 1, axis=1))
    return jnp.where(lane == LANES - 1, 0.0, pltpu.roll(x, LANES - 1, axis=1))


def step_kernel(
    slabs, images,
    feats_hbm, taps_hbm, embed_hbm, row_hbm, qkv_hbm, out_hbm, proj_hbm, dino_hbm,
    gfeat_ref, gproj_ref, gconv_ref, loss_ref,
    feats, taps_s, embed_s, row_s, w_own, out_w, proj_w, dino, load_sems,
    taps48, resp_g, terms, terms_all, stack, tokens, emb, xw, tstack, mt, ep,
    inv_s, gct, k_s, v_s, qt, s_s, e_s, r_s, attt, att, base, residb, gzp, gt_aug, gt, ds_s,
    gk_s, gv_s, gqt, yr, spread, spread_all, vs,
    cbuf, crecv, cfull, gp, r1, h1, r2, h2, r3, gpo, loss_s,
    dino_sems, t_send, t_recv, a_send, a_recv, s_send, s_recv,
    c_send, c_recv, d_send, d_recv, p1_sems, p2_sems, p3_send, p3_recv, a3_send, a3_recv,
    a2_sems, a1_sems, a0_sems,
):
    slab = lax.axis_index("slab")
    image = lax.axis_index("img")
    core = lax.rem(slab, 2)
    chip = slab // 2
    partner = {"slab": slab + 1 - 2 * core, "img": image}
    devices = slabs * images
    me = slab * images + image
    depth = images // 2
    east, north = lax.rem(image, 2), image // 2
    first = chip + core * (east - chip)
    second = east + core * (chip - east)
    hop1 = {"slab": slab + (1 - core) * (2 - 4 * chip), "img": image + core * (1 - 2 * east)}
    hop2 = {"slab": slab + core * (2 - 4 * chip), "img": image + (1 - core) * (1 - 2 * east)}
    width = out_w.shape[0]
    half = width // 2
    full = tokens.shape[1]
    block = dino.shape[1]
    own = 2 * block
    npairs = half // PAIR
    f_rows = emb.shape[0]

    def anyone(j):
        return {"slab": j // images, "img": lax.rem(j, images)}

    def level(j):
        return {"slab": slab, "img": j * 2 + east}

    def remote(src, dst, send, recv, device):
        return pltpu.make_async_remote_copy(
            src_ref=src, dst_ref=dst, send_sem=send, recv_sem=recv,
            device_id=device, device_id_type=MESH_ID)

    def others(count, self_index, body):
        def run(step, _):
            body(lax.rem(self_index + step, count))
            return 0

        lax.fori_loop(1, count, run, 0)

    barrier = pltpu.get_barrier_semaphore()
    loads = [pltpu.make_async_copy(feats_hbm, feats, load_sems.at[0])]
    for j in range(3):
        loads.append(pltpu.make_async_copy(
            qkv_hbm.at[:, pl.ds(pl.multiple_of(j * width + core * half, LANES), half)],
            w_own.at[j], load_sems.at[1 + j]))
    loads.append(pltpu.make_async_copy(proj_hbm, proj_w, load_sems.at[4]))
    loads.append(pltpu.make_async_copy(
        out_hbm.at[pl.ds(pl.multiple_of(core * half, 8), half)],
        out_w.at[pl.ds(pl.multiple_of(core * half, 8), half)], load_sems.at[5]))
    loads.append(pltpu.make_async_copy(dino_hbm, dino.at[core], load_sems.at[6]))
    loads.append(pltpu.make_async_copy(taps_hbm, taps_s, load_sems.at[7]))
    loads.append(pltpu.make_async_copy(embed_hbm, embed_s, load_sems.at[8]))
    loads.append(pltpu.make_async_copy(row_hbm, row_s, load_sems.at[9]))
    loads.append(pltpu.make_async_copy(
        out_hbm.at[pl.ds(pl.multiple_of((1 - core) * half, 8), half)],
        out_w.at[pl.ds(pl.multiple_of((1 - core) * half, 8), half)], load_sems.at[10]))
    for i in (7, 8, 0, 9, 4, 5, 1, 2, 3, 6, 10):
        loads[i].start()

    others(devices, me, lambda j: pl.semaphore_signal(
        barrier, inc=1, device_id=anyone(j), device_id_type=MESH_ID))

    vs[...] = jnp.zeros_like(vs)
    loads[7].wait()
    loads[8].wait()
    for kx in range(3):
        for ky in range(3):
            vs[kx * 16 + ky * 4 : kx * 16 + ky * 4 + 4, : feats.shape[1]] = (
                taps_s[ky * 3 + kx].astype(F32))
    taps48[...] = vs[:, : feats.shape[1]].astype(BF16)
    for dy in range(2):
        for dx in range(2):
            emb[dx * 8 + dy * 4 : dx * 8 + dy * 4 + 4, :] = (
                embed_s[dy * 8 + dx * 4 : dy * 8 + dx * 4 + 4, :].astype(F32))

    loads[0].wait()
    resp = contract_last(taps48[...], feats[...])
    rows = resp.shape[1] // LANES
    for r in range(rows):
        cut = slice(r * LANES, (r + 1) * LANES)
        resp_g[r] = resp[16:32, cut] + shifted(resp[0:16, cut], 1) + shifted(resp[32:48, cut], -1)
    tiles = rows // 2 + 2
    for k in range(tiles):
        for dy in range(2):
            h = 2 * (k - 1) + dy
            total = None
            for ky in range(3):
                r = h + ky - 1
                if 0 <= r < rows:
                    part = resp_g[r, ky * 4 : ky * 4 + 4, :]
                    total = part if total is None else total + part
            if total is None:
                total = jnp.zeros((4, LANES), F32)
            terms[k, dy * 4 : dy * 4 + 4, :] = total

    pl.semaphore_wait(barrier, devices - 1)
    t_copies = []
    for d in range(1, slabs):
        peer = lax.rem(slab + d, slabs)
        t_copies.append(remote(
            terms, terms_all.at[slab], t_send, t_recv, {"slab": peer, "img": image}))
    for c in t_copies:
        c.start()
    loads[6].wait()
    dino_copy = remote(dino_hbm, dino.at[core], dino_sems.at[0], dino_sems.at[1], partner)
    dino_copy.start()
    terms_all[slab] = terms[...]

    loads[4].wait()
    ep[...] = plain(emb[...].astype(BF16), proj_w[...])
    loads[5].wait()
    mt[...] = plain(
        out_w[pl.ds(pl.multiple_of(core * half, 8), half), :], proj_w[...]).astype(BF16)
    ebar = jnp.mean(emb[...], 1, keepdims=True)
    ecent = emb[...] - ebar
    gram = lax.dot_general(
        ecent, ecent, (((1,), (1,)), ((), ())), precision=lax.Precision.HIGHEST,
        preferred_element_type=F32)
    loads[9].wait()
    row = row_s[...]
    gain = 1.0 + row[:, width:]
    stack_l = jnp.concatenate(
        [emb[...] * gain, gain, row[:, :width], jnp.zeros((6, width), F32)], 0)
    parts = jnp.concatenate(split3(stack_l), 0)
    for j in range(3):
        loads[1 + j].wait()
        prod = plain(parts, w_own[j])
        xw[j] = prod[0:24] + prod[24:48] + prod[48:72]

    few = slabs - 1
    halo_wait = remote(
        terms_all.at[pl.ds(0, few)], terms_all.at[pl.ds(0, few)], t_send, t_recv, partner)
    halo_wait.wait_recv()

    per = rows // 2
    for i in range(per * slabs):
        p, k = divmod(i, per)
        lat = terms_all[p, k + 1]
        if k == 0 and p > 0:
            lat = lat + terms_all[p - 1, per + 1]
        if k == per - 1 and p < slabs - 1:
            lat = lat + terms_all[p + 1, 0]
        stack[(i // 2) * 8 : (i // 2) * 8 + 8, (i % 2) * LANES : (i % 2 + 1) * LANES] = (
            lat * latent_scale)
    spots = iota((2 * LANES, 2 * LANES), 0)
    dests = iota((2 * LANES, 2 * LANES), 1)
    hit = jnp.logical_and(
        lax.shift_right_logical(spots, 7) == lax.shift_right_logical(dests & 127, 6),
        (spots & 127) == 2 * (dests & 63) + lax.shift_right_logical(dests, 7))
    select = jnp.where(hit, 1.0, 0.0).astype(BF16)
    lines = stack.shape[0]
    moved = plain(jnp.concatenate(split3(stack[...]), 0), select)
    moved = moved[0:lines] + moved[lines : 2 * lines] + moved[2 * lines :]
    for i2 in range(lines // 8):
        for dx in range(2):
            tokens[dx * 8 : dx * 8 + 8, i2 * LANES : (i2 + 1) * LANES] = (
                moved[i2 * 8 : i2 * 8 + 8, dx * LANES : (dx + 1) * LANES])
    tok = tokens[...]
    emb_b = emb[...].astype(BF16)
    tok3 = jnp.concatenate(split3(tok), 0)
    emb3 = jnp.concatenate([emb_b] * 3, 0)
    invs = []
    for b in range(full // 256):
        st = contract_first(emb3, tok3[:, b * 256 : (b + 1) * 256])
        cent = st - jnp.mean(st, 0, keepdims=True)
        invs.append(lax.rsqrt(jnp.mean(cent * cent, 0, keepdims=True) + norm_eps))
    inv = jnp.concatenate(invs, 1)
    inv_s[...] = inv
    tn = tok * inv
    tokens[...] = tn
    gct[...] = lax.dot_general(
        gram, tn, (((1,), (0,)), ((), ())), precision=lax.Precision.HIGHEST,
        preferred_element_type=F32) * (1.0 / width)
    tn_hi, tn_lo = split2(tn)
    ones = jnp.where(iota((16, full), 0) < 2, 1.0, 0.0).astype(BF16)
    tstack[...] = jnp.concatenate([tn_hi, tn_hi, tn_lo, ones], 0)

    def basis(j):
        b = xw[j, 0:16, :] - ebar * xw[j, 16:17, :]
        b_hi, b_lo = split2(b)
        s_hi, s_lo = split2(xw[j, 17:18, :])
        line = iota((16, half), 0)
        bias = jnp.where(line == 0, s_hi.astype(F32), jnp.where(line == 1, s_lo.astype(F32), 0.0))
        return jnp.concatenate([b_hi, b_lo, b_hi, bias.astype(BF16)], 0)

    bk, bv, bq = basis(1), basis(2), basis(0)
    lane = iota((256, PAIR), 1)
    for b in range(full // 256):
        cut = slice(b * 256, (b + 1) * 256)
        ts = tstack[:, cut]
        kk = contract_first(ts, bk)
        vv = contract_first(ts, bv)
        for p in range(npairs):
            k_s[p, cut, :] = kk[:, p * PAIR : (p + 1) * PAIR].astype(BF16)
            vp = vv[:, p * PAIR : (p + 1) * PAIR]
            v_s[2 * p, cut, :] = jnp.where(
                lane < HEAD_DIM, vp, jnp.where(lane < HEAD_DIM + 2, 1.0, 0.0)).astype(BF16)
            v_s[2 * p + 1, cut, :] = jnp.where(
                lane >= HEAD_DIM, vp, jnp.where(lane < 2, 1.0, 0.0)).astype(BF16)
    chip_cut = pl.ds(pl.multiple_of(chip * own, LANES), own)
    qq = contract_first(bq, tstack[:, chip_cut]).astype(BF16) * BF16(HEAD_DIM ** -0.5)
    blank = jnp.zeros((HEAD_DIM, own), BF16)
    for p in range(npairs):
        qt[2 * p] = jnp.concatenate([qq[p * PAIR : p * PAIR + HEAD_DIM], blank], 0)
        qt[2 * p + 1] = jnp.concatenate([blank, qq[p * PAIR + HEAD_DIM : (p + 1) * PAIR]], 0)

    def att_copy(p):
        return remote(att.at[core, p], att.at[core, p], a_send, a_recv, partner)

    units = [(p, b, h) for p in range(npairs) for b in range(own // 256) for h in range(2)]

    def scores(i):
        p, b, h = units[i]
        s = plain(k_s[p], qt[2 * p + h, :, b * 256 : (b + 1) * 256])
        s_s[i % 3] = s
        return jnp.max(s, 0, keepdims=True)

    def weigh(i, top):
        p, b, h = units[i]
        e_s[2 * p + h, :, b * 256 : (b + 1) * 256] = jnp.exp(s_s[i % 3] - top).astype(BF16)

    def gather(i, kept):
        p, b, h = units[i]
        cut = slice(b * 256, (b + 1) * 256)
        o = contract_first(v_s[2 * p + h], e_s[2 * p + h, :, cut])
        at = HEAD_DIM if h == 0 else 0
        r = 1.0 / o[at : at + 1]
        r_s[p, h : h + 1, cut] = r
        kept[h] = o[h * HEAD_DIM : (h + 1) * HEAD_DIM] * r
        if h == 1:
            both = jnp.concatenate(kept, 0)
            attt[p, :, cut] = both.astype(BF16)
            att[core, p, cut, :] = both.T.astype(BF16)
            if b == own // 256 - 1:
                att_copy(p).start()

    kept, top = [None, None], scores(0)
    for i in range(len(units) + 1):
        later = scores(i + 1) if i + 1 < len(units) else None
        if i < len(units):
            weigh(i, top)
        if i > 0:
            gather(i - 1, kept)
        top = later
    tstack[0:48, :] = tok3
    cuts = [slice(b * 256, (b + 1) * 256) for b in range(own // 256)]

    def outward(side, cut):
        a = jnp.concatenate([att[side, p, cut, :] for p in range(npairs)], 1)
        return plain(a, out_w[pl.ds(pl.multiple_of(side * half, 8), half), :])

    for b, cut in enumerate(cuts):
        piece = pl.ds(pl.multiple_of(chip * own + b * 256, LANES), 256)
        base[cut, :] = contract_first(tstack[0:48, piece], emb3) + outward(core, cut)
    spread[...] = jnp.zeros_like(spread)
    vs[...] = jnp.zeros_like(vs)
    ep_parts = jnp.concatenate(split2(ep[...]), 0)
    loads[10].wait()
    dino_copy.wait_recv()
    att_wait = remote(att.at[core], att.at[core], a_send, a_recv, partner)
    att_wait.wait_recv()
    loss = jnp.zeros((1, 1), F32)
    for b, cut in enumerate(cuts):
        rb = (base[cut, :] + outward(1 - core, cut)).astype(BF16)
        residb[cut, :] = rb
        zp = plain(rb, proj_w[...])
        d = dino[b].astype(F32)
        norm_p = jnp.sqrt(jnp.sum(zp * zp, -1, keepdims=True) + cosine_eps)
        norm_t = jnp.sqrt(jnp.sum(d * d, -1, keepdims=True) + cosine_eps)
        cos = jnp.sum(zp * d, -1, keepdims=True) / (norm_p * norm_t)
        gzp[cut, :] = (zp * (cos / (norm_p * norm_p)) - d / (norm_p * norm_t)).astype(BF16)
        loss = loss + jnp.sum(1.0 - cos, 0, keepdims=True) * 0.5
    loss_s[...] = loss

    rh = residb[:, pl.ds(pl.multiple_of(core * half, LANES), half)]
    chunks, wide = gp.shape[0], gp.shape[-1]
    ranks = range(chunks)

    def p1(k):
        return remote(gp.at[k, 1 - first], r1.at[k], p1_sems.at[chunks], p1_sems.at[k], hop1)

    def p2(k):
        return remote(h1.at[k, 1 - second], r2.at[k], p2_sems.at[chunks], p2_sems.at[k], hop2)

    def p3(k, j):
        return remote(h2.at[k, j], r3.at[k, north], p3_send, p3_recv.at[k], level(j))

    def p3_wait(k):
        some = r3.at[k, pl.ds(0, depth - 1)]
        return remote(some, some, p3_send, p3_recv.at[k], partner)

    def a3(k, j):
        mine = gpo.at[core, k, first, second, north]
        return remote(mine, mine, a3_send, a3_recv.at[k], level(j))

    def a3_wait(k):
        some = gpo.at[core, k, first, second, pl.ds(0, depth - 1)]
        return remote(some, some, a3_send, a3_recv.at[k], partner)

    def a2(k, there):
        return remote(
            gpo.at[core, k, first, second], gpo.at[core, k, first, there],
            a2_sems.at[chunks], a2_sems.at[k], hop2)

    def a1(k, there):
        return remote(
            gpo.at[core, k, first], gpo.at[core, k, there],
            a1_sems.at[chunks], a1_sems.at[k], hop1)

    def a0(k, part):
        some = gpo.at[core, k, part]
        return remote(some, some, a0_sems.at[chunks], a0_sems.at[k], partner)

    def a0_wait(k):
        some = gpo.at[1 - core, k]
        return remote(some, some, a0_sems.at[chunks], a0_sems.at[k], partner)

    def add1(k):
        p1(k).wait_recv()
        h1[k] = (gp[k, first].astype(F32) + r1[k].astype(F32)).astype(BF16)
        p2(k).start()

    def add2(k):
        p2(k).wait_recv()
        h2[k] = (h1[k, second].astype(F32) + r2[k].astype(F32)).astype(BF16)
        others(depth, north, lambda j: p3(k, j).start())

    def add3(k):
        p3_wait(k).wait_recv()
        total = lax.fori_loop(
            1, depth, lambda i, acc: acc + r3[k, lax.rem(north + i, depth)].astype(F32),
            h2[k, north].astype(F32))
        gpo[core, k, first, second, north] = total.astype(BF16)
        others(depth, north, lambda j: a3(k, j).start())

    def give3(k):
        a3_wait(k).wait_recv()
        a2(k, second).start()

    def give2(k):
        a2(k, 1 - second).wait_recv()
        a1(k, first).start()
        a0(k, first).start()

    def give1(k):
        a1(k, 1 - first).wait_recv()
        a0(k, 1 - first).start()

    for k in ranks:
        part = contract_first(rh, gzp[:, k * wide : (k + 1) * wide]).astype(BF16)
        gp[k] = part.reshape(gp.shape[1:])
        p1(k).start()

    gatt = contract_last(mt[...], gzp[...]).astype(BF16)
    yrr = contract_last(ep_parts, gzp[...])
    yr[...] = (yrr[0:f_rows] + yrr[f_rows : 2 * f_rows]) * 0.5
    line16 = iota((16, own), 0)
    for p in range(npairs):
        g = gatt[p * PAIR : (p + 1) * PAIR].astype(F32)
        prod = g * attt[p].astype(F32)
        for h in range(2):
            cut = slice(h * HEAD_DIM, (h + 1) * HEAD_DIM)
            r = r_s[p, h : h + 1, :]
            delta = jnp.sum(prod[cut], 0, keepdims=True) * r
            d_hi, d_lo = split2(-delta)
            gr = (g[cut] * r).astype(BF16)
            extra = jnp.where(
                line16 == 0, d_hi.astype(F32), jnp.where(line16 == 1, d_lo.astype(F32), 0.0))
            fill = jnp.concatenate(
                [extra.astype(BF16), jnp.zeros((HEAD_DIM - 16, own), BF16)], 0)
            gt_aug[2 * p + h] = jnp.concatenate([gr, fill] if h == 0 else [fill, gr], 0)
            gt[2 * p + h] = jnp.concatenate([gr, blank] if h == 0 else [blank, gr], 0)

    def backward(p, _):
        q_pair = jnp.concatenate([qt[2 * p], qt[2 * p + 1]], 1)
        g_pair = jnp.concatenate([gt[2 * p], gt[2 * p + 1]], 1)
        for c in range(full // 256):
            cut = slice(c * 256, (c + 1) * 256)
            dss, es = [], []
            for h in range(2):
                dp = plain(v_s[2 * p + h, cut, :], gt_aug[2 * p + h])
                e = e_s[2 * p + h, cut, :]
                ds = (e.astype(F32) * dp).astype(BF16)
                ds_s[h, cut, :] = ds
                dss.append(ds)
                es.append(e)
            gk_s[p, cut, :] = contract_last(jnp.concatenate(dss, 1), q_pair).astype(BF16)
            gv_s[p, cut, :] = contract_last(jnp.concatenate(es, 1), g_pair).astype(BF16)
        outs = []
        for h in range(2):
            o = contract_first(k_s[p], ds_s[h])
            outs.append(o[h * HEAD_DIM : (h + 1) * HEAD_DIM] * HEAD_DIM ** -0.5)
        gqt[pl.ds(pl.multiple_of(p * PAIR, PAIR), PAIR), :] = jnp.concatenate(outs, 0).astype(BF16)
        for k in ranks:
            pl.when(p == k)(functools.partial(add1, k))
        for k in ranks[:2]:
            pl.when(p == k + 2)(functools.partial(add2, k))
        return 0

    lax.fori_loop(0, npairs, backward, 0)

    def weights(j):
        return jnp.concatenate(split2(xw[j]), 0)

    inv = inv_s[...]
    tn = tokens[...]
    y = contract_last(weights(1), jnp.concatenate([gk_s[p] for p in range(npairs)], 1))
    y = y + contract_last(weights(2), jnp.concatenate([gv_s[p] for p in range(npairs)], 1))
    y = y[0:24] + y[24:48]
    yq = plain(weights(0), gqt[...])
    yq = yq[0:24] + yq[24:48]

    def back(y, inv, tn, gct):
        yc = y[0:16] - ebar * y[16:17]
        return inv * (yc - gct * jnp.sum(tn * yc, 0, keepdims=True))

    sp = back(y, inv, tn, gct[...])
    sq = back(yq, inv_s[:, chip_cut], tokens[:, chip_cut], gct[:, chip_cut]) + yr[...]
    for t in range(full // LANES):
        spread[t + 1] = sp[:, t * LANES : (t + 1) * LANES]
    for t in range(own // LANES):
        spread[chip * (own // LANES) + t + 1] += sq[:, t * LANES : (t + 1) * LANES]
    strip = block // LANES
    s_copies = []
    for d in range(1, slabs):
        peer = lax.rem(slab + d, slabs)
        s_copies.append(remote(
            spread.at[pl.ds(peer * strip, strip + 2)], spread_all.at[slab],
            s_send, s_recv, {"slab": peer, "img": image}))
    for c in s_copies:
        c.start()
    spread_all[slab] = spread[pl.ds(slab * strip, strip + 2)]
    for k in ranks[2:]:
        add2(k)
    add3(0)
    back_wait = remote(
        spread_all.at[pl.ds(0, few)], spread_all.at[pl.ds(0, few)], s_send, s_recv, partner)
    back_wait.wait_recv()

    add3(1)
    cells = []
    for t in range(strip + 2):
        g = spread_all[0, t]
        for p in range(1, slabs):
            g = g + spread_all[p, t]
        g = (g * latent_scale).astype(BF16)
        cells.append(jnp.concatenate([g[0:8], g[8:16]], 1))
    stack[0 : 8 * (strip + 2), :] = contract_last(jnp.concatenate(cells, 0), select)
    for r in range(rows):
        cut = slice(r * LANES, (r + 1) * LANES)
        for ky in range(3):
            h = r + 1 - ky + 4
            t, rest = divmod(h, 4)
            p, dy = divmod(rest, 2)
            vs[16 + ky * 4 : 20 + ky * 4, cut] = stack[
                t * 8 + dy * 4 : t * 8 + dy * 4 + 4, p * LANES : (p + 1) * LANES]
        mid_view = vs[16:32, cut]
        vs[0:16, cut] = shifted(mid_view, -1)
        vs[32:48, cut] = shifted(mid_view, 1)
    views = vs[...].astype(BF16)
    conv_part = plain(views, feats[...])
    cbuf[...] = jnp.zeros_like(cbuf)
    for i in range(TAPS // 8):
        for j in range(4):
            cbuf[i * 4 + j] = conv_part[
                i * 8 : i * 8 + 8, j * LANES : (j + 1) * LANES].astype(BF16)
    loss_hi, loss_lo = split2(loss_s[...])
    cbuf[TAPS // 2] = jnp.where(
        iota((8, LANES), 0) == 0, loss_hi.astype(F32), loss_lo.astype(F32)).astype(BF16)
    used = TAPS // 2 + 1

    def owners(body):
        def run(j, _):
            pl.when(j != me)(lambda: body(j))
            return 0

        lax.fori_loop(0, used, run, 0)

    def scatter(j):
        return remote(cbuf.at[j], crecv.at[me], c_send, c_recv, anyone(j))

    def tiles_of(ref, count, send, recv):
        return remote(ref.at[pl.ds(0, count)], ref.at[pl.ds(0, count)], send, recv, partner)

    def by_role(body):
        pl.when(me < used)(lambda: body(used - 1))
        pl.when(me >= used)(lambda: body(used))

    def share(j):
        return remote(cfull.at[me], cfull.at[me], d_send, d_recv, anyone(j))

    owners(lambda j: scatter(j).start())
    for k in ranks[2:]:
        add3(k)
    for i in range(rows * LANES // 256):
        cut = slice(i * 256, (i + 1) * 256)
        gfeat_ref[cut, :] = contract_first(views[:, cut], taps48[...]).astype(BF16)
    for k in ranks[:2]:
        give3(k)

    @pl.when(me < used)
    def _():
        crecv[me] = cbuf[me]
        tiles_of(crecv, devices - 1, c_send, c_recv).wait_recv()
        total = jnp.sum(crecv[...].astype(F32), 0)
        high = total.astype(BF16)
        cfull[me, 0] = high
        cfull[me, 1] = (total - high.astype(F32)).astype(BF16)
        others(devices, me, lambda j: share(j).start())

    give2(0)
    for k in ranks[2:]:
        give3(k)
    for k in ranks[1:]:
        give2(k)
    halo_wait.wait_send()
    dino_copy.wait_send()
    att_wait.wait_send()
    back_wait.wait_send()
    by_role(lambda count: tiles_of(cbuf, count, c_send, c_recv).wait_send())
    remote(r1, r1, p1_sems.at[chunks], p1_sems.at[0], partner).wait_send()
    remote(r2, r2, p2_sems.at[chunks], p2_sems.at[0], partner).wait_send()
    every = r3.at[:, pl.ds(0, depth - 1)]
    remote(every, every, p3_send, p3_recv.at[0], partner).wait_send()
    by_role(lambda count: tiles_of(cfull, count, d_send, d_recv).wait_recv())
    for i in range(TAPS // 8):
        for j in range(4):
            tile = cfull[i * 4 + j].astype(F32)
            vs[i * 8 : i * 8 + 8, j * LANES : (j + 1) * LANES] = tile[0] + tile[1]
    for kx in range(3):
        for ky in range(3):
            gconv_ref[ky * 3 + kx] = vs[kx * 16 + ky * 4 : kx * 16 + ky * 4 + 4, : 4 * LANES]
    tile = cfull[TAPS // 2].astype(F32)
    tile = tile[0] + tile[1]
    loss_ref[...] = (tile[0:1, 0:1] + tile[1:2, 0:1]) * (1.0 / (devices * block))

    def store(side, k):
        gproj_ref[side, :, k * wide : (k + 1) * wide] = (
            gpo[side, k].astype(F32).reshape(half, wide))

    for k in ranks:
        give1(k)
        store(core, k)
        if k > 0:
            a0_wait(k - 1).wait_recv()
            store(1 - core, k - 1)
    a0_wait(chunks - 1).wait_recv()
    store(1 - core, chunks - 1)
    @pl.when(me < used)
    def _():
        tiles_of(cfull, devices - 1, d_send, d_recv).wait_send()

    for ref, send, recv in (
        (gpo.at[core, :, first, second, pl.ds(0, depth - 1)], a3_send, a3_recv.at[0]),
        (gpo.at[core, :, first, second], a2_sems.at[chunks], a2_sems.at[0]),
        (gpo.at[core, :, first], a1_sems.at[chunks], a1_sems.at[0]),
        (gpo.at[core], a0_sems.at[chunks], a0_sems.at[0]),
    ):
        remote(ref, ref, send, recv, partner).wait_send()


def finish_kernel(*refs):
    count = (len(refs) - 1) // 2
    sems = refs[-1]
    pieces = 4
    copies = []
    for i in range(count):
        left, right = refs[i], refs[count + i]
        cuts = pieces if len(left.shape) == 2 and left.shape[0] > 8 else 1
        lines = left.shape[0] // cuts
        for j in range(cuts):
            copies.append(pltpu.make_async_copy(
                left.at[j * lines : (j + 1) * lines], right.at[j * lines : (j + 1) * lines],
                sems.at[i, j]))
    for c in copies:
        c.start()
    for c in copies:
        c.wait()


def local(feats, labels, conv_w, embed_w, mod_table, qkv_w, out_w, proj_w, dino):
    _, rows, cols, chans = feats.shape
    width = qkv_w.shape[0]
    deep = proj_w.shape[1]
    slabs = lax.axis_size("slab")
    images = lax.axis_size("img")
    devices = slabs * images
    half = width // 2
    block = dino.shape[1]
    own = 2 * block
    full = slabs * block
    heads = half // HEAD_DIM
    pairs = half // PAIR
    features = embed_w.shape[0]
    taps = conv_w.transpose(0, 2, 1)
    row = lax.dynamic_slice_in_dim(mod_table, labels[0], 1, 0).astype(F32)
    depth = images // 2
    wide = 2 * LANES
    piece = half // (4 * depth)
    chunks = deep // wide
    hbm = pl.BlockSpec(memory_space=pltpu.HBM)
    vmem = pl.BlockSpec(memory_space=pltpu.VMEM)
    dma = pltpu.SemaphoreType.DMA
    strip = block // LANES
    V = pltpu.VMEM
    scratch = [
        V((rows * cols, chans), BF16), V(taps.shape, BF16), V(embed_w.shape, BF16),
        V((1, 2 * width), F32), V((3, width, half), BF16), V((width, width), BF16),
        V((width, deep), BF16), V((2, block, deep), BF16), dma((11,)),
        V((TAPS, chans), BF16), V((rows, 16, LANES), F32), V((rows // 2 + 2, 8, LANES), F32),
        V((slabs, rows // 2 + 2, 8, LANES), F32), V((rows * slabs // 4 * 8, 2 * LANES), F32),
        V((features, full), F32), V((features, width), F32), V((3, 24, half), F32),
        V((64, full), BF16), V((half, deep), BF16), V((features, deep), F32),
        V((1, full), F32), V((features, full), F32), V((pairs, full, PAIR), BF16),
        V((heads, full, PAIR), BF16), V((heads, PAIR, own), BF16), V((3, full, 256), F32),
        V((heads, full, own), BF16),
        V((pairs, 2, own), F32), V((pairs, PAIR, own), BF16), V((2, pairs, own, PAIR), BF16), V((own, width), F32),
        V((own, width), BF16), V((own, deep), BF16), V((heads, PAIR, own), BF16),
        V((heads, PAIR, own), BF16), V((2, full, own), BF16),
        V((pairs, full, PAIR), BF16), V((pairs, full, PAIR), BF16), V((half, own), BF16),
        V((features, own), F32), V((full // LANES + 2, features, LANES), F32),
        V((slabs, strip + 2, features, LANES), F32), V((TAPS, rows * cols), F32),
        V((devices, 8, LANES), BF16), V((devices, 8, LANES), BF16), V((devices, 2, 8, LANES), BF16),
        V((chunks, 2, 2, depth, piece, wide), BF16), V((chunks, 2, depth, piece, wide), BF16),
        V((chunks, 2, depth, piece, wide), BF16), V((chunks, depth, piece, wide), BF16),
        V((chunks, depth, piece, wide), BF16), V((chunks, depth, piece, wide), BF16),
        V((2, chunks, 2, 2, depth, piece, wide), BF16), V((1, 1), F32),
        dma((2,)), dma, dma, dma, dma, dma, dma, dma, dma, dma, dma, dma((chunks + 1,)),
        dma((chunks + 1,)), dma, dma((chunks,)), dma, dma((chunks,)), dma((chunks + 1,)),
        dma((chunks + 1,)), dma((chunks + 1,)),
    ]
    shapes = [
        jax.ShapeDtypeStruct((rows * cols, chans), BF16),
        jax.ShapeDtypeStruct((2, half, deep), F32),
        jax.ShapeDtypeStruct((9, conv_w.shape[2], chans), F32),
        jax.ShapeDtypeStruct((1, 1), F32),
    ]
    given = (feats.reshape(rows * cols, chans), taps, embed_w, row, qkv_w, out_w, proj_w, dino[0])
    made = pl.pallas_call(
        functools.partial(step_kernel, slabs, images),
        out_shape=shapes,
        in_specs=[hbm] * 8,
        out_specs=[vmem] * 4,
        scratch_shapes=scratch,
        compiler_params=pltpu.CompilerParams(
            collective_id=0, has_side_effects=True, vmem_limit_bytes=GRANT),
        name="step",
    )(*[pltpu.with_memory_space_constraint(x, pltpu.HBM) for x in given])
    made = [made[0], made[1].reshape(width, deep), made[2], made[3]]
    gfeat, gproj, gconv, loss = pl.pallas_call(
        finish_kernel,
        in_specs=[vmem] * 4,
        out_specs=[hbm] * 4,
        out_shape=[jax.ShapeDtypeStruct(m.shape, m.dtype) for m in made],
        scratch_shapes=[dma((4, 4))],
        compiler_params=pltpu.CompilerParams(vmem_limit_bytes=8 * 1024 * 1024),
        name="finish",
    )(*made)
    return (
        gfeat.reshape(feats.shape), gproj.reshape(width, deep), gconv.transpose(0, 2, 1),
        loss.reshape(()),
    )


def solution(mesh):
    in_specs = (
        P("img", "slab", None, None),
        P("img"),
        P(),
        P(),
        P(),
        P(),
        P(),
        P(),
        P("img", "slab", None),
    )
    out_specs = (P("img", "slab", None, None), P(), P(), P())
    return jax.shard_map(local, mesh=mesh, in_specs=in_specs, out_specs=out_specs, check_vma=False)
```
